1024 devices in a mesh: face: 256 (over y, z, core), sub: 4 (over x).
Axes of the slice: x: 4, y: 8, z: 16, core: 2. Of those that a mesh axis runs over, the one named last changes fastest.
Arguments:
- prognostic: bfloat16 [3, 65536, 16, 128], P(None, ('face', 'sub')), may hold values from -4 to 4
- metric: float32 [4, 65536, 16], P(None, ('face', 'sub')), may hold values from -0.35 to 1.6, as said below
- coriolis: float32 [65536, 16], P(('face', 'sub')), may hold values from -1.5 to 1.5
- node_point: int32 [65536, 16], P(('face', 'sub')), may hold values from 0 to 678, as said below
- send_point: int32 [217088], P(('face', 'sub')), may hold values from 0 to 678, as said below
- recv_point: int32 [217088], P(('face', 'sub')), may hold values from 0 to 678, as said below
Outputs:
- advanced: bfloat16 [3, 65536, 16, 128], P(None, ('face', 'sub'))
The draws below stay inside these ranges and needn't reach their ends.
Inputs may be any that keep to these rules, and one draw needn't show every extreme that they name: `node_point`: each device's numbers are its 679 local points; element nodes that are the same point of the surface on one device carry the same number. `send_point`: on every device the 212 slots form groups in this order: 7 slots of offset +1, 7 of offset -1, 97 of offset +16, 97 of offset -16, then one slot each of offsets 16 + 1, -16 - 1, 15, 1 - 16. A slot names the sender's point that the device at curve index d + o, taken modulo 1024, shares. Every slot is used. `recv_point`: slot s of device d names the local point that is the same surface point as the sender's slot s, the sender being the device at d minus the slot's group offset modulo 1024. The copies of every shared point are linked between every two devices that hold them. `metric`: entries 0 and 3 lie in [0.6, 1.6], entries 1 and 2 in [-0.35, 0.35].
All inputs are finite; a program needn't handle non-finite values.
Results may differ from the reference program's by a relative error of at most 0.007.
Values sent between devices are 32-bit elements; how exact they have to be, the bound alone decides.
A program may use at most 32 MiB of HBM per device.

```python
import math
import jax
import jax.numpy as jnp
import numpy as np
from jax import lax

BX = 32
BY = 2
LEV = 128
ELEMS = 64
BLOCKS = 1024
ELEMENTS = 65536
LAP = 16
PTS = 679
LINKS = 212


def link_grid_points():
    grid_width = 3 * BX + 1
    grid_height = 3 * BY + 1
    sender = []
    receiver = []
    for height in range(grid_height):
        sender.append(height * grid_width + 3 * BX)
        receiver.append(height * grid_width)
    for height in range(grid_height):
        sender.append(height * grid_width)
        receiver.append(height * grid_width + 3 * BX)
    for column in range(grid_width):
        sender.append(3 * BY * grid_width + column)
        receiver.append(column)
    for column in range(grid_width):
        sender.append(column)
        receiver.append(3 * BY * grid_width + column)
    sender.append(3 * BY * grid_width + 3 * BX)
    receiver.append(0)
    sender.append(0)
    receiver.append(3 * BY * grid_width + 3 * BX)
    sender.append(3 * BY * grid_width)
    receiver.append(3 * BX)
    sender.append(3 * BX)
    receiver.append(3 * BY * grid_width)
    return (np.array(sender, np.int32), np.array(receiver, np.int32))


def mesh_tables(key):
    base = jax.random.fold_in(key, 4242)
    key_elem, key_rot, key_point = jax.random.split(base, 3)
    elements = BX * BY
    placement_order = jax.vmap(lambda sub_key: jax.random.permutation(sub_key, elements))(jax.random.split(key_elem, BLOCKS)).astype(jnp.int32)
    rotation = jax.random.randint(key_rot, (BLOCKS, elements), 0, 4).astype(jnp.int32)[..., None]
    relabel = jax.vmap(lambda sub_key: jax.random.permutation(sub_key, PTS))(jax.random.split(key_point, BLOCKS)).astype(jnp.int32)
    across = placement_order % BX
    upward = placement_order // BX
    node_index = jnp.arange(16, dtype=jnp.int32)
    node_row = node_index // 4
    node_col = node_index % 4
    rot_col = jnp.where(rotation == 0, node_col, jnp.where(rotation == 1, 3 - node_row, jnp.where(rotation == 2, 3 - node_col, node_row)))
    rot_row = jnp.where(rotation == 0, node_row, jnp.where(rotation == 1, node_col, jnp.where(rotation == 2, 3 - node_row, 3 - node_col)))
    grid_index = (3 * upward[..., None] + rot_row) * (3 * BX + 1) + 3 * across[..., None] + rot_col
    node_table = jnp.take_along_axis(relabel, grid_index.reshape(BLOCKS, elements * 16).astype(jnp.int32), axis=1)
    sender, receiver = link_grid_points()
    send_table = relabel[:, jnp.asarray(sender)].reshape(-1).astype(jnp.int32)
    recv_table = relabel[:, jnp.asarray(receiver)].reshape(-1).astype(jnp.int32)
    return (node_table.reshape(ELEMENTS, 16).astype(jnp.int32), send_table, recv_table)


def draw_node_point(key, part):
    return mesh_tables(key)[0]


def draw_send_point(key, part):
    return mesh_tables(key)[1]


def draw_recv_point(key, part):
    return mesh_tables(key)[2]


def draw_metric(key, part):
    key_diag, key_off = jax.random.split(jax.random.fold_in(key, 17), 2)
    diagonal = jnp.exp(jax.random.uniform(key_diag, (2, ELEMENTS, 16), jnp.float32, math.log(0.6), math.log(1.6)))
    off_diag = jax.random.uniform(key_off, (2, ELEMENTS, 16), jnp.float32, -0.35, 0.35)
    diagonal = jnp.clip(diagonal, 0.6, 1.6)
    return jnp.stack([diagonal[0], off_diag[0], off_diag[1], diagonal[1]]).astype(jnp.float32)


def block_levels(own_key, shape, cuts, least, high):
    level, own = 1.0, jax.random.fold_in(own_key, 6)
    for position, parts in cuts:
        heights = jnp.exp(jax.random.uniform(jax.random.fold_in(own, position), (parts,), jnp.float32, least / len(cuts), high / len(cuts)))
        level = level * jnp.repeat(heights, shape[position] // parts).reshape([-1 if axis == position else 1 for axis in range(len(shape))])
    return level


def gaussian(own_key, dims, spread, most, cuts=(), held_as=jnp.bfloat16):
    loudness = block_levels(own_key, dims, cuts, -0.22, 0.18) if cuts else 1.0
    values = jax.random.normal(own_key, dims, jnp.float32) * spread * loudness
    return jnp.minimum(jnp.maximum(values, -most), most).astype(held_as)


def setup_inputs(seed: int = 0) -> dict:
    streams_of = jax.random.split(jax.random.key(seed), 7)
    prognostic = gaussian(streams_of[0], (3, ELEMENTS, 16, LEV), 1.0, 4.0, ((1, 1024),))
    metric = draw_metric(jax.random.fold_in(streams_of[6], 71), 0)
    coriolis = jnp.clip(jax.random.uniform(streams_of[2], (ELEMENTS, 16), jnp.float32, -1.5, 1.5) * block_levels(streams_of[2], (ELEMENTS, 16), ((0, 1024),), -0.4, 0.0), -1.5, 1.5)
    node_point = draw_node_point(jax.random.fold_in(streams_of[6], 71), 0)
    send_point = draw_send_point(jax.random.fold_in(streams_of[6], 71), 0)
    recv_point = draw_recv_point(jax.random.fold_in(streams_of[6], 71), 0)
    return dict(prognostic=prognostic, metric=metric, coriolis=coriolis, node_point=node_point, send_point=send_point, recv_point=recv_point)


STEP_SIZE = 0.1

def gll_tables():
    abscissa = np.array([-1.0, -math.sqrt(0.2), math.sqrt(0.2), 1.0])
    legendre = 0.5 * (5.0 * abscissa * abscissa * abscissa - 3.0 * abscissa)
    derivative = np.zeros((4, 4))
    for target in range(4):
        for source in range(4):
            if target != source:
                derivative[target, source] = legendre[target] / (legendre[source] * (abscissa[target] - abscissa[source]))
    derivative[0, 0] = -3.0
    derivative[3, 3] = 3.0
    weights = np.array([1.0, 5.0, 5.0, 1.0]) / 6.0
    return (derivative, weights)

def along_cols(values, derivative):
    return jnp.einsum('aj,erjl->eral', derivative, values, precision=lax.Precision.HIGHEST)

def along_rows(values, derivative):
    return jnp.einsum('aj,ejcl->eacl', derivative, values, precision=lax.Precision.HIGHEST)

def element_tendency(fields, metric, coriolis):
    elements = fields.shape[1]
    levels = fields.shape[3]
    deriv_table, weight_table = gll_tables()
    derivative = jnp.asarray(deriv_table, dtype=jnp.float32)
    weights = jnp.asarray(weight_table, dtype=jnp.float32)
    shaped = fields.reshape(3, elements, 4, 4, levels)
    veloc_one = shaped[0]
    veloc_two = shaped[1]
    geopot = shaped[2]
    inverse = metric.reshape(4, elements, 4, 4, 1)
    inv_aa = inverse[0]
    inv_ab = inverse[1]
    inv_ba = inverse[2]
    inv_bb = inverse[3]
    jacobian_inv = inv_aa * inv_bb - inv_ab * inv_ba
    energy = 0.5 * (veloc_one * veloc_one + veloc_two * veloc_two) + geopot
    ref_one = along_cols(energy, derivative)
    ref_two = along_rows(energy, derivative)
    grad_one = inv_aa * ref_one + inv_ba * ref_two
    grad_two = inv_ab * ref_one + inv_bb * ref_two
    cov_one = (inv_bb * veloc_one - inv_ba * veloc_two) / jacobian_inv
    cov_two = (inv_aa * veloc_two - inv_ab * veloc_one) / jacobian_inv
    vorticity = jacobian_inv * (along_cols(cov_two, derivative) - along_rows(cov_one, derivative))
    absolute = vorticity + coriolis.reshape(elements, 4, 4, 1)
    flux_one = geopot * veloc_one
    flux_two = geopot * veloc_two
    contra_one = (inv_aa * flux_one + inv_ab * flux_two) / jacobian_inv
    contra_two = (inv_ba * flux_one + inv_bb * flux_two) / jacobian_inv
    divergence = jacobian_inv * (along_cols(contra_one, derivative) + along_rows(contra_two, derivative))
    tendency = jnp.stack([absolute * veloc_two - grad_one, -absolute * veloc_one - grad_two, -divergence])
    mass_weight = (weights[:, None] * weights[None, :])[None] / jacobian_inv[..., 0]
    return (tendency.reshape(3, elements, 16, levels), mass_weight.reshape(elements, 16))

def link_groups(lap_blocks):
    side_points = 3 * BY + 1
    top_points = 3 * BX + 1
    group_sizes = [(1, side_points), (-1, side_points), (lap_blocks, top_points), (-lap_blocks, top_points), (lap_blocks + 1, 1), (-lap_blocks - 1, 1), (lap_blocks - 1, 1), (1 - lap_blocks, 1)]
    groups = []
    first_slot = 0
    for offset, slot_count in group_sizes:
        groups.append((offset, first_slot, slot_count))
        first_slot = first_slot + slot_count
    return groups

def block_terms(prognostic, metric, coriolis, node_point, device_index):
    first_elem = (device_index * ELEMS).astype(jnp.int32)
    fields = lax.dynamic_slice_in_dim(prognostic, first_elem, ELEMS, 1).astype(jnp.float32)
    local_metric = lax.dynamic_slice_in_dim(metric, first_elem, ELEMS, 1)
    local_coriolis = lax.dynamic_slice_in_dim(coriolis, first_elem, ELEMS, 0)
    point_ids = lax.dynamic_slice_in_dim(node_point, first_elem, ELEMS, 0).reshape(-1)
    tendency, mass_weight = element_tendency(fields, local_metric, local_coriolis)
    weighted = (tendency * mass_weight[None, :, :, None]).reshape(3, ELEMS * 16, LEV)
    partial_value = jnp.zeros((3, PTS, LEV), jnp.float32).at[:, point_ids, :].add(weighted)
    weight = jnp.zeros((PTS,), jnp.float32).at[point_ids].add(mass_weight.reshape(-1))
    return (fields, point_ids, partial_value, weight)

def reference(prognostic, metric, coriolis, node_point, send_point, recv_point):
    device_list = jnp.arange(BLOCKS, dtype=jnp.int32)

    def outgoing_of(device_index):
        fields, point_ids, partial_value, weight = block_terms(prognostic, metric, coriolis, node_point, device_index)
        link_ids = lax.dynamic_slice_in_dim(send_point, (device_index * LINKS).astype(jnp.int32), LINKS, 0)
        return (partial_value[:, link_ids, :], weight[link_ids])
    sent_values, sent_weight = lax.map(outgoing_of, device_list)
    groups = link_groups(LAP)

    def advance(device_index, collected):
        fields, point_ids, partial_value, weight = block_terms(prognostic, metric, coriolis, node_point, device_index)
        link_ids = lax.dynamic_slice_in_dim(recv_point, (device_index * LINKS).astype(jnp.int32), LINKS, 0)
        arrived_values = []
        arrived_weight = []
        for offset, first_slot, slot_count in groups:
            source = jnp.mod(device_index - offset, BLOCKS).astype(jnp.int32)
            values_from = lax.dynamic_index_in_dim(sent_values, source, 0, keepdims=False)
            weight_from = lax.dynamic_index_in_dim(sent_weight, source, 0, keepdims=False)
            arrived_values.append(values_from[:, first_slot:first_slot + slot_count, :])
            arrived_weight.append(weight_from[first_slot:first_slot + slot_count])
        total = partial_value.at[:, link_ids, :].add(jnp.concatenate(arrived_values, axis=1))
        total_weight = weight.at[link_ids].add(jnp.concatenate(arrived_weight, axis=0))
        averaged = total[:, point_ids, :] / total_weight[point_ids][None, :, None]
        advanced = (fields + STEP_SIZE * averaged.reshape(3, ELEMS, 16, LEV)).astype(jnp.bfloat16)
        first_elem = (device_index * ELEMS).astype(jnp.int32)
        return lax.dynamic_update_slice_in_dim(collected, advanced, first_elem, 1)
    result = jnp.zeros((3, ELEMENTS, 16, LEV), jnp.bfloat16)
    return lax.fori_loop(0, BLOCKS, advance, result)
```

```python
import functools
import math

import jax
import jax.numpy as jnp
import numpy as np
from jax import lax
from jax.experimental import pallas as pl
from jax.experimental.pallas import tpu as pltpu
from jax.sharding import PartitionSpec as P

MESH = pl.DeviceIdType.MESH
BX = 32
BY = 2
ELEMS = BX * BY
NODES = ELEMS * 16
LEV = 128
SIDE = 3 * BY + 1
TOP = 3 * BX + 1
LINKS = 2 * SIDE + 2 * TOP + 4
STEP_SIZE = 0.1
BLK = 16

GROUPS = (
    (2, 2 * SIDE, TOP, 0, 104),
    (3, 2 * SIDE + TOP, TOP, 128, 104),
    (0, 0, SIDE, 104, 8),
    (1, SIDE, SIDE, 232, 8),
    (4, 2 * SIDE + 2 * TOP, 1, 112, 8),
    (5, 2 * SIDE + 2 * TOP + 1, 1, 240, 8),
    (6, 2 * SIDE + 2 * TOP + 2, 1, 120, 8),
    (7, 2 * SIDE + 2 * TOP + 3, 1, 248, 8),
)
ROWS = 256


def gll_tables():
    abscissa = np.array([-1.0, -math.sqrt(0.2), math.sqrt(0.2), 1.0])
    legendre = 0.5 * (5.0 * abscissa * abscissa * abscissa - 3.0 * abscissa)
    derivative = np.zeros((4, 4))
    for target in range(4):
        for source in range(4):
            if target != source:
                derivative[target, source] = legendre[target] / (
                    legendre[source] * (abscissa[target] - abscissa[source])
                )
    derivative[0, 0] = -3.0
    derivative[3, 3] = 3.0
    weights = np.array([1.0, 5.0, 5.0, 1.0]) / 6.0
    return derivative, weights


DERIV, GLL = gll_tables()
EV0 = float(0.5 * (DERIV[0, 0] + DERIV[0, 3]))
EV1 = float(0.5 * (DERIV[1, 0] + DERIV[1, 3]))
OD00 = float(0.5 * (DERIV[0, 0] - DERIV[0, 3]))
OD01 = float(0.5 * (DERIV[0, 1] - DERIV[0, 2]))
OD10 = float(0.5 * (DERIV[1, 0] - DERIV[1, 3]))
OD11 = float(0.5 * (DERIV[1, 1] - DERIV[1, 2]))


def derive4(s):
    o0 = s[0] - s[3]
    o1 = s[1] - s[2]
    q = (s[0] + s[3]) - (s[1] + s[2])
    h0 = OD00 * o0 + OD01 * o1
    h1 = OD10 * o0 + OD11 * o1
    g0 = EV0 * q
    g1 = EV1 * q
    return [h0 + g0, h1 + g1, h1 - g1, h0 - g0]


def along_cols(s):
    out = []
    for r in range(4):
        out += derive4(s[4 * r : 4 * r + 4])
    return out


def along_rows(s):
    out = [None] * 16
    for c in range(4):
        for r, value in enumerate(derive4(s[c::4])):
            out[4 * r + c] = value
    return out


NODE_W = [float(GLL[n // 4] * GLL[n % 4]) for n in range(16)]


def lane_iota(shape):
    return lax.broadcasted_iota(jnp.int32, shape, len(shape) - 1)


def padded_slots(ref):
    x = jnp.concatenate(
        [jnp.broadcast_to(ref[...], (8, LINKS)), jnp.full((8, ROWS - LINKS), -1, jnp.int32)], axis=1
    )
    lane = lane_iota((8, ROWS))
    out = jnp.full((8, ROWS), -1, jnp.int32)
    for _, first, count, row, _ in GROUPS:
        moved = pltpu.roll(x, (row - first) % ROWS, 1)
        out = jnp.where((lane >= row) & (lane < row + count), moved, out)
    return out


def one_hot(col, row):
    return jnp.where(col == row, 1.0, 0.0).astype(jnp.bfloat16)


def kernel(
    sizes,
    prog_hbm, met_hbm, cor_hbm, np_hbm, sp_hbm, rp_hbm,
    out_ref,
    prog_v, met_v, cor_v, np_v, sp_v, rp_v,
    f_v, ct_v, w_v, s_v, a_v, r_v, acc_v, inv_v, ids_v, out_b, in_b,
    in_sem, send_sem, recv_sem,
):
    n_face, n_sub = sizes
    total = n_face * n_sub
    lap = 4 * n_sub
    offsets = (1, -1, lap, -lap, lap + 1, -lap - 1, lap - 1, 1 - lap)
    me = lax.axis_index("face") * n_sub + lax.axis_index("sub")

    def device(offset):
        t = lax.rem(me + (offset + total), total)
        return (t // n_sub, lax.rem(t, n_sub))

    loads = []
    for i, (src, dst) in enumerate(
        ((np_hbm, np_v), (sp_hbm, sp_v), (rp_hbm, rp_v), (met_hbm, met_v), (cor_hbm, cor_v))
    ):
        loads.append(pltpu.make_async_copy(src, dst, in_sem.at[i]))
    for f in range(3):
        loads.append(pltpu.make_async_copy(prog_hbm.at[f], prog_v.at[f], in_sem.at[5 + f]))
    for load in loads:
        load.start()

    barrier = pltpu.get_barrier_semaphore()
    for offset in offsets:
        pl.semaphore_signal(barrier, inc=1, device_id=device(offset), device_id_type=MESH)

    def remote(f, g):
        group, _, _, row, rows = g
        return pltpu.make_async_remote_copy(
            src_ref=out_b.at[f, pl.ds(row, rows)],
            dst_ref=in_b.at[f, pl.ds(row, rows)],
            send_sem=send_sem.at[f, group],
            recv_sem=recv_sem.at[f, group],
            device_id=device(offsets[group]),
            device_id_type=MESH,
        )

    for load in loads[:3]:
        load.wait()
    ids = np_v[...]
    ids2 = jnp.concatenate([ids, ids], axis=1)
    ids_v[...] = ids2
    half = lane_iota((8, LEV)) < ELEMS
    id_rows = []
    for j in range(8):
        even = jnp.broadcast_to(ids2[2 * j : 2 * j + 1], (8, LEV))
        odd = jnp.broadcast_to(ids2[2 * j + 1 : 2 * j + 2], (8, LEV))
        id_rows.append(jnp.where(half, even, odd)[0:1])
    send_row = padded_slots(sp_v)
    recv_row = padded_slots(rp_v)
    for chunk in range(2):
        col = jnp.transpose(
            jnp.broadcast_to(send_row[0:1, 128 * chunk : 128 * chunk + 128], (128, 128))
        )
        for j in range(8):
            s_v[128 * chunk : 128 * chunk + 128, 128 * j : 128 * j + 128] = one_hot(col, id_rows[j])

    for load in loads[3:5]:
        load.wait()
    m_a, m_b, m_e, m_g = (met_v[i] for i in range(4))
    inverse = 1.0 / (m_a * m_g - m_b * m_e)
    node = lax.broadcasted_iota(jnp.int32, (16, ELEMS), 0)
    wr = jnp.where((node < 4) | (node >= 12), float(GLL[0]), float(GLL[1]))
    wc = jnp.where((node % 4 == 0) | (node % 4 == 3), float(GLL[0]), float(GLL[1]))
    mass = wr * wc * inverse
    coefs = jnp.concatenate(
        [m_a * inverse, m_b * inverse, m_e * inverse, m_g * inverse, mass * cor_v[...], mass, mass, mass],
        axis=0,
    )
    ct_v[...] = jnp.transpose(coefs)

    for f in range(3):
        loads[5 + f].wait()
        f_v[NODES * f : NODES * f + NODES] = prog_v[f].astype(jnp.float32)

    def fields_of(k):
        base = k * (BLK * 16)
        return [
            [f_v[pl.ds(f * NODES + base + n, BLK, stride=16), :] for n in range(16)]
            for f in range(3)
        ]

    def spread(ct, q, n):
        i = q * 16 + n
        return jnp.broadcast_to(ct[:, i : i + 1], (BLK, LEV))

    def rows_of(k, n):
        return pl.ds(pl.multiple_of(n * ELEMS + k * BLK, BLK), BLK)

    def first_pass(k, carry):
        u1, u2, phi = fields_of(k)
        ct = ct_v[pl.ds(pl.multiple_of(k * BLK, BLK), BLK), :]
        con1, con2 = [], []
        low = lane_iota((BLK, LEV)) < 64
        for n in range(16):
            f1 = phi[n] * u1[n]
            f2 = phi[n] * u2[n]
            con1.append(spread(ct, 0, n) * f1 + spread(ct, 1, n) * f2)
            con2.append(spread(ct, 2, n) * f1 + spread(ct, 3, n) * f2)
            mass = spread(ct, 5, n)
            high = mass.astype(jnp.bfloat16).astype(jnp.float32)
            w_v[rows_of(k, n), 128:256] = jnp.where(low, high, mass - high).astype(jnp.bfloat16)
        d1 = along_cols(con1)
        d2 = along_rows(con2)
        for n in range(16):
            w_v[rows_of(k, n), 0:128] = (-NODE_W[n] * (d1[n] + d2[n])).astype(jnp.bfloat16)
        return carry

    lax.fori_loop(0, ELEMS // BLK, first_pass, 0)

    sent = jnp.dot(s_v[...], w_v[:, 0:256], preferred_element_type=jnp.float32)
    out_b[0] = sent[:, 0:128]
    weight = sent[:, 128:256]
    weight = weight + pltpu.roll(weight, 64, 1)
    diagonal = lax.broadcasted_iota(jnp.int32, (128, 128), 0) == lane_iota((128, 128))
    for chunk in range(2):
        row = jnp.sum(
            jnp.where(diagonal, weight[128 * chunk : 128 * chunk + 128], 0.0), axis=0, keepdims=True
        )
        for _, _, count, first, _ in GROUPS:
            if first // 128 == chunk:
                out_b[0, first + count : first + count + 1, :] = row
    pl.semaphore_wait(barrier, len(offsets))
    for g in GROUPS:
        remote(0, g).start()

    def second_pass(k, carry):
        u1, u2, phi = fields_of(k)
        ct = ct_v[pl.ds(pl.multiple_of(k * BLK, BLK), BLK), :]
        energy, cov1, cov2 = [], [], []
        for n in range(16):
            energy.append(0.5 * (u1[n] * u1[n] + u2[n] * u2[n]) + phi[n])
            cov1.append(spread(ct, 3, n) * u1[n] - spread(ct, 2, n) * u2[n])
            cov2.append(spread(ct, 0, n) * u2[n] - spread(ct, 1, n) * u1[n])
        curl1 = along_cols(cov2)
        curl2 = along_rows(cov1)
        e1 = along_cols(energy)
        e2 = along_rows(energy)
        for n in range(16):
            eta = NODE_W[n] * (curl1[n] - curl2[n]) + spread(ct, 4, n)
            grad1 = spread(ct, 0, n) * e1[n] + spread(ct, 2, n) * e2[n]
            grad2 = spread(ct, 1, n) * e1[n] + spread(ct, 3, n) * e2[n]
            w_v[rows_of(k, n), 256:384] = (eta * u2[n] - NODE_W[n] * grad1).astype(jnp.bfloat16)
            w_v[rows_of(k, n), 384:512] = (-eta * u1[n] - NODE_W[n] * grad2).astype(jnp.bfloat16)
        return carry

    lax.fori_loop(0, ELEMS // BLK, second_pass, 0)
    sent = jnp.dot(s_v[...], w_v[:, 256:512], preferred_element_type=jnp.float32)
    for f in (1, 2):
        out_b[f] = sent[:, 128 * (f - 1) : 128 * f]
        for g in GROUPS:
            remote(f, g).start()

    def table(e, carry):
        x = ids_v[...]
        col = jnp.broadcast_to(pltpu.roll(x, LEV - e, 1)[:, 0:1], (16, LEV))
        rows = pl.ds(pl.multiple_of(e * 16, 16), 16)
        for j in range(8):
            a_v[rows, 128 * j : 128 * j + 128] = one_hot(col, id_rows[j])
        for chunk in range(2):
            r_v[rows, 128 * chunk : 128 * chunk + 128] = one_hot(
                col, recv_row[0:1, 128 * chunk : 128 * chunk + 128]
            )
        return carry

    lax.fori_loop(0, ELEMS, table, 0)

    def gather(i, carry):
        rows = pl.ds(pl.multiple_of(i * 256, 256), 256)
        acc_v[rows, :] = jnp.dot(a_v[rows, :], w_v[...], preferred_element_type=jnp.float32)
        return carry

    lax.fori_loop(0, NODES // 256, gather, 0)

    def finish(f, cols):
        def body(i, carry):
            rows = pl.ds(pl.multiple_of(i * 256, 256), 256)
            got = jnp.dot(
                r_v[rows, :], in_b[f].astype(jnp.bfloat16), preferred_element_type=jnp.float32
            )
            got = got + acc_v[rows, cols : cols + 128]
            field = prog_v[(f + 2) % 3, rows, :].astype(jnp.float32)
            out_ref[(f + 2) % 3, rows, :] = (field + got * inv_v[rows, :]).astype(jnp.bfloat16)
            return carry

        lax.fori_loop(0, NODES // 256, body, 0)

    for g in GROUPS:
        remote(0, g).wait_recv()
    lane = lane_iota((1, 128))
    low = lane_iota((128, 128)) < 64
    blocks = []
    for chunk in range(2):
        row = jnp.zeros((1, 128), jnp.float32)
        for _, _, count, first, _ in GROUPS:
            if first // 128 == chunk:
                at = first % 128
                row = jnp.where(
                    (lane >= at) & (lane < at + count), in_b[0, first + count : first + count + 1, :], row
                )
        col = jnp.transpose(jnp.broadcast_to(row, (128, 128)))
        high = col.astype(jnp.bfloat16).astype(jnp.float32)
        blocks.append(jnp.where(low, high, col - high).astype(jnp.bfloat16))
    arrived = jnp.concatenate(blocks, axis=0)

    def weights(i, carry):
        rows = pl.ds(pl.multiple_of(i * 256, 256), 256)
        w = jnp.dot(r_v[rows, :], arrived, preferred_element_type=jnp.float32)
        w = w + acc_v[rows, 128:256]
        w = w + pltpu.roll(w, 64, 1)
        inv_v[rows, :] = STEP_SIZE / w
        return carry

    lax.fori_loop(0, NODES // 256, weights, 0)
    finish(0, 0)
    for f in (1, 2):
        for g in GROUPS:
            remote(f, g).wait_recv()
        finish(f, 128 + 128 * f)
    for f in range(3):
        for g in GROUPS:
            remote(f, g).wait_send()


def solution(mesh):
    sizes = (mesh.shape["face"], mesh.shape["sub"])

    def local(prognostic, metric, coriolis, node_point, send_point, recv_point):
        result = pl.pallas_call(
            functools.partial(kernel, sizes),
            out_shape=jax.ShapeDtypeStruct((3, NODES, LEV), jnp.bfloat16),
            in_specs=[pl.BlockSpec(memory_space=pl.ANY)] * 6,
            out_specs=pl.BlockSpec(memory_space=pltpu.VMEM),
            scratch_shapes=[
                pltpu.VMEM((3, NODES, LEV), jnp.bfloat16),
                pltpu.VMEM((4, 16, ELEMS), jnp.float32),
                pltpu.VMEM((16, ELEMS), jnp.float32),
                pltpu.VMEM((16, ELEMS), jnp.int32),
                pltpu.VMEM((1, LINKS), jnp.int32),
                pltpu.VMEM((1, LINKS), jnp.int32),
                pltpu.VMEM((3 * NODES, LEV), jnp.float32),
                pltpu.VMEM((ELEMS, 128), jnp.float32),
                pltpu.VMEM((NODES, 512), jnp.bfloat16),
                pltpu.VMEM((ROWS, NODES), jnp.bfloat16),
                pltpu.VMEM((NODES, NODES), jnp.bfloat16),
                pltpu.VMEM((NODES, ROWS), jnp.bfloat16),
                pltpu.VMEM((NODES, 512), jnp.float32),
                pltpu.VMEM((NODES, LEV), jnp.float32),
                pltpu.VMEM((16, LEV), jnp.int32),
                pltpu.VMEM((3, ROWS, LEV), jnp.float32),
                pltpu.VMEM((3, ROWS, LEV), jnp.float32),
                pltpu.SemaphoreType.DMA((8,)),
                pltpu.SemaphoreType.DMA((3, 8)),
                pltpu.SemaphoreType.DMA((3, 8)),
            ],
            compiler_params=pltpu.CompilerParams(collective_id=0, has_side_effects=True),
        )(
            prognostic.reshape(3, NODES, LEV),
            jnp.transpose(metric, (0, 2, 1)),
            jnp.transpose(coriolis),
            jnp.transpose(node_point),
            send_point.reshape(1, LINKS),
            recv_point.reshape(1, LINKS),
        )
        return result.reshape(3, ELEMS, 16, LEV)

    placed = (
        P(None, ("face", "sub"), None, None),
        P(None, ("face", "sub"), None),
        P(("face", "sub"), None),
        P(("face", "sub"), None),
        P(("face", "sub")),
        P(("face", "sub")),
    )
    return jax.shard_map(
        local,
        mesh=mesh,
        in_specs=placed,
        out_specs=P(None, ("face", "sub"), None, None),
        check_vma=False,
    )
```

```python
import functools
import math

import jax
import jax.numpy as jnp
import numpy as np
from jax import lax
from jax.experimental import pallas as pl
from jax.experimental.pallas import tpu as pltpu
from jax.sharding import PartitionSpec as P

MESH = pl.DeviceIdType.MESH
BX = 32
BY = 2
ELEMS = BX * BY
NODES = ELEMS * 16
LEV = 128
SIDE = 3 * BY + 1
TOP = 3 * BX + 1
LINKS = 2 * SIDE + 2 * TOP + 4
STEP_SIZE = 0.1
BLK = 16
BLOCKS = ELEMS // BLK
BROWS = 16 * BLK

GROUPS = (
    (2, 2 * SIDE, TOP, 0),
    (3, 2 * SIDE + TOP, TOP, 128),
    (0, 0, SIDE, 104),
    (1, SIDE, SIDE, 232),
    (4, 2 * SIDE + 2 * TOP, 1, 112),
    (5, 2 * SIDE + 2 * TOP + 1, 1, 240),
    (6, 2 * SIDE + 2 * TOP + 2, 1, 120),
    (7, 2 * SIDE + 2 * TOP + 3, 1, 248),
)
ROWS = 256


def gll_tables():
    abscissa = np.array([-1.0, -math.sqrt(0.2), math.sqrt(0.2), 1.0])
    legendre = 0.5 * (5.0 * abscissa * abscissa * abscissa - 3.0 * abscissa)
    derivative = np.zeros((4, 4))
    for target in range(4):
        for source in range(4):
            if target != source:
                derivative[target, source] = legendre[target] / (
                    legendre[source] * (abscissa[target] - abscissa[source])
                )
    derivative[0, 0] = -3.0
    derivative[3, 3] = 3.0
    weights = np.array([1.0, 5.0, 5.0, 1.0]) / 6.0
    return derivative, weights


DERIV, GLL = gll_tables()
EV0 = float(0.5 * (DERIV[0, 0] + DERIV[0, 3]))
EV1 = float(0.5 * (DERIV[1, 0] + DERIV[1, 3]))
OD00 = float(0.5 * (DERIV[0, 0] - DERIV[0, 3]))
OD01 = float(0.5 * (DERIV[0, 1] - DERIV[0, 2]))
OD10 = float(0.5 * (DERIV[1, 0] - DERIV[1, 3]))
OD11 = float(0.5 * (DERIV[1, 1] - DERIV[1, 2]))


def derive4(s):
    o0 = s[0] - s[3]
    o1 = s[1] - s[2]
    q = (s[0] + s[3]) - (s[1] + s[2])
    h0 = OD00 * o0 + OD01 * o1
    h1 = OD10 * o0 + OD11 * o1
    g0 = EV0 * q
    g1 = EV1 * q
    return [h0 + g0, h1 + g1, h1 - g1, h0 - g0]


def along_cols(s):
    out = []
    for r in range(4):
        out += derive4(s[4 * r : 4 * r + 4])
    return out


def along_rows(s):
    out = [None] * 16
    for c in range(4):
        for r, value in enumerate(derive4(s[c::4])):
            out[4 * r + c] = value
    return out


NODE_W = [float(GLL[n // 4] * GLL[n % 4]) for n in range(16)]


def lane_iota(shape):
    return lax.broadcasted_iota(jnp.int32, shape, len(shape) - 1)


def padded_slots(ref):
    x = jnp.concatenate(
        [jnp.broadcast_to(ref[...], (8, LINKS)), jnp.full((8, ROWS - LINKS), -1, jnp.int32)], axis=1
    )
    lane = lane_iota((8, ROWS))
    out = jnp.full((8, ROWS), -1, jnp.int32)
    for _, first, count, row in GROUPS:
        moved = pltpu.roll(x, (row - first) % ROWS, 1)
        out = jnp.where((lane >= row) & (lane < row + count), moved, out)
    return out


def one_hot(col, row):
    return jnp.where(col == row, 1.0, 0.0).astype(jnp.bfloat16)


def kernel(
    sizes,
    prog_hbm, met_hbm, cor_hbm, np_hbm, sp_hbm, rp_hbm,
    out_ref,
    prog_v, met_v, cor_v, np_v, sp_v, rp_v,
    f_v, ct_v, co_v, w_v, s_v, a_v, r_v, acc_v, inv_v, ids_v, out_b, in_b,
    in_sem, send_sem, recv_sem,
):
    n_face, n_sub = sizes
    total = n_face * n_sub
    lap = 4 * n_sub
    offsets = (1, -1, lap, -lap, lap + 1, -lap - 1, lap - 1, 1 - lap)
    me = lax.axis_index("face") * n_sub + lax.axis_index("sub")

    def device(offset):
        t = lax.rem(me + (offset + total), total)
        return (t // n_sub, lax.rem(t, n_sub))

    barrier = pltpu.get_barrier_semaphore()
    loads = []
    for i, (src, dst) in enumerate(
        ((np_hbm, np_v), (sp_hbm, sp_v), (rp_hbm, rp_v), (met_hbm, met_v), (cor_hbm, cor_v))
    ):
        loads.append(pltpu.make_async_copy(src, dst, in_sem.at[i]))
    for k in range(BLOCKS):
        for f in range(3):
            rows = pl.ds(BROWS * k, BROWS)
            loads.append(
                pltpu.make_async_copy(
                    prog_hbm.at[f, rows], prog_v.at[f, rows], in_sem.at[5 + 3 * k + f]
                )
            )
    for load in loads:
        load.start()
    for offset in offsets:
        pl.semaphore_signal(barrier, inc=1, device_id=device(offset), device_id_type=MESH)

    def remote(f, g):
        group, _, count, row = g
        rows = count + 1 if f == 0 else count
        return pltpu.make_async_remote_copy(
            src_ref=out_b.at[f, pl.ds(row, rows)],
            dst_ref=in_b.at[f, pl.ds(row, rows)],
            send_sem=send_sem.at[f, group],
            recv_sem=recv_sem.at[f, group],
            device_id=device(offsets[group]),
            device_id_type=MESH,
        )

    edges = sorted((row, row + count) for _, _, count, row in GROUPS)
    for f in range(3):
        for (_, end), nxt in zip(edges, [e[0] for e in edges[1:]] + [ROWS]):
            end = end + 1 if f == 0 else end
            if nxt > end:
                in_b[f, end:nxt, :] = jnp.zeros((nxt - end, LEV), jnp.float32)

    for load in loads[:3]:
        load.wait()
    ids = np_v[...]
    ids2 = jnp.concatenate([ids, ids], axis=1)
    ids_v[...] = ids2
    rolled = [ids2 if i == 0 else pltpu.roll(ids2, 16 * i, 1) for i in range(4)]
    sub = lax.broadcasted_iota(jnp.int32, (8, LEV), 0)
    own = sub == lane_iota((8, LEV)) // BLK
    id_rows = []
    for k in range(BLOCKS):
        for h in range(2):
            pick = rolled[(-k) % 4][8 * h : 8 * h + 8]
            for i in range(1, 4):
                pick = jnp.where(sub % 4 == i, rolled[(i - k) % 4][8 * h : 8 * h + 8], pick)
            id_rows.append(jnp.sum(jnp.where(own, pick, 0), axis=0, keepdims=True))
    send_row = padded_slots(sp_v)
    recv_row = padded_slots(rp_v)
    for chunk in range(2):
        col = jnp.transpose(
            jnp.broadcast_to(send_row[0:1, 128 * chunk : 128 * chunk + 128], (128, 128))
        )
        for j in range(8):
            s_v[128 * chunk : 128 * chunk + 128, 128 * j : 128 * j + 128] = one_hot(col, id_rows[j])

    for load in loads[3:5]:
        load.wait()
    m_a, m_b, m_e, m_g = (met_v[i] for i in range(4))
    inverse = 1.0 / (m_a * m_g - m_b * m_e)
    node = lax.broadcasted_iota(jnp.int32, (16, ELEMS), 0)
    wr = jnp.where((node < 4) | (node >= 12), float(GLL[0]), float(GLL[1]))
    wc = jnp.where((node % 4 == 0) | (node % 4 == 3), float(GLL[0]), float(GLL[1]))
    mass = wr * wc * inverse
    coefs = jnp.concatenate(
        [m_a * inverse, m_b * inverse, m_e * inverse, m_g * inverse, mass * cor_v[...], mass, mass, mass],
        axis=0,
    )
    ct_v[...] = jnp.transpose(coefs)

    def rows_of(k, n):
        first = k * BROWS + n * BLK
        return pl.ds(first if isinstance(first, int) else pl.multiple_of(first, BLK), BLK)

    ct = ct_v[...]
    low = lane_iota((ELEMS, LEV)) < 64
    for n in range(16):
        for q in range(6):
            wide = jnp.broadcast_to(ct[:, q * 16 + n : q * 16 + n + 1], (ELEMS, LEV))
            if q == 5:
                high = wide.astype(jnp.bfloat16).astype(jnp.float32)
                wide = jnp.where(low, high, wide - high).astype(jnp.bfloat16)
            for k in range(BLOCKS):
                part = wide[BLK * k : BLK * k + BLK]
                if q == 5:
                    w_v[rows_of(k, n), 128:256] = part
                else:
                    co_v[q, rows_of(k, n), :] = part

    weight = jnp.dot(s_v[...], w_v[:, 128:256], preferred_element_type=jnp.float32)
    weight = weight + pltpu.roll(weight, 64, 1)
    diagonal = lax.broadcasted_iota(jnp.int32, (128, 128), 0) == lane_iota((128, 128))
    for chunk in range(2):
        row = jnp.sum(
            jnp.where(diagonal, weight[128 * chunk : 128 * chunk + 128], 0.0), axis=0, keepdims=True
        )
        for _, _, count, first in GROUPS:
            if first // 128 == chunk:
                out_b[0, first + count : first + count + 1, :] = row

    def fields_of(k):
        return [
            [f_v[pl.ds(f * NODES + k * BROWS + n, BLK, stride=16), :] for n in range(16)]
            for f in range(3)
        ]

    sent = jnp.zeros((ROWS, LEV), jnp.float32)
    for k in range(BLOCKS):
        for f in range(3):
            loads[5 + 3 * k + f].wait()
            f_v[f * NODES + k * BROWS : f * NODES + k * BROWS + BROWS] = prog_v[
                f, BROWS * k : BROWS * k + BROWS
            ].astype(jnp.float32)
        u1, u2, phi = fields_of(k)
        con1, con2 = [], []
        for n in range(16):
            f1 = phi[n] * u1[n]
            f2 = phi[n] * u2[n]
            con1.append(co_v[0, rows_of(k, n), :] * f1 + co_v[1, rows_of(k, n), :] * f2)
            con2.append(co_v[2, rows_of(k, n), :] * f1 + co_v[3, rows_of(k, n), :] * f2)
        d1 = along_cols(con1)
        d2 = along_rows(con2)
        for n in range(16):
            w_v[rows_of(k, n), 0:128] = (-NODE_W[n] * (d1[n] + d2[n])).astype(jnp.bfloat16)
        sent = sent + jnp.dot(
            s_v[:, BROWS * k : BROWS * k + BROWS],
            w_v[BROWS * k : BROWS * k + BROWS, 0:128],
            preferred_element_type=jnp.float32,
        )
    for _, _, count, row in GROUPS:
        out_b[0, row : row + count, :] = sent[row : row + count]
    pl.semaphore_wait(barrier, len(offsets))
    for g in GROUPS:
        remote(0, g).start()

    def second_pass(k, carry):
        u1, u2, phi = fields_of(k)
        energy, cov1, cov2 = [], [], []
        for n in range(16):
            rows = rows_of(k, n)
            energy.append(0.5 * (u1[n] * u1[n] + u2[n] * u2[n]) + phi[n])
            cov1.append(co_v[3, rows, :] * u1[n] - co_v[2, rows, :] * u2[n])
            cov2.append(co_v[0, rows, :] * u2[n] - co_v[1, rows, :] * u1[n])
        curl1 = along_cols(cov2)
        curl2 = along_rows(cov1)
        e1 = along_cols(energy)
        e2 = along_rows(energy)
        for n in range(16):
            rows = rows_of(k, n)
            eta = NODE_W[n] * (curl1[n] - curl2[n]) + co_v[4, rows, :]
            grad1 = co_v[0, rows, :] * e1[n] + co_v[2, rows, :] * e2[n]
            grad2 = co_v[1, rows, :] * e1[n] + co_v[3, rows, :] * e2[n]
            w_v[rows, 256:384] = (eta * u2[n] - NODE_W[n] * grad1).astype(jnp.bfloat16)
            w_v[rows, 384:512] = (-eta * u1[n] - NODE_W[n] * grad2).astype(jnp.bfloat16)
        return carry

    lax.fori_loop(0, BLOCKS, second_pass, 0)
    sent = jnp.dot(s_v[...], w_v[:, 256:512], preferred_element_type=jnp.float32)
    for f in (1, 2):
        out_b[f] = sent[:, 128 * (f - 1) : 128 * f]
        for g in GROUPS:
            remote(f, g).start()

    def table(i, carry):
        x = pltpu.roll(ids_v[...], LEV - 8 * i, 1)
        for lane in range(8):
            col = jnp.broadcast_to(x[:, lane : lane + 1], (16, LEV))
            rows = pl.ds(pl.multiple_of(i * 128 + lane * 16, 16), 16)
            for j in range(8):
                a_v[rows, 128 * j : 128 * j + 128] = one_hot(col, id_rows[j])
            for chunk in range(2):
                r_v[rows, 128 * chunk : 128 * chunk + 128] = one_hot(
                    col, recv_row[0:1, 128 * chunk : 128 * chunk + 128]
                )
        return carry

    lax.fori_loop(0, ELEMS // 8, table, 0)

    def gather(i, carry):
        rows = pl.ds(pl.multiple_of(i * 256, 256), 256)
        acc_v[rows, :] = jnp.dot(a_v[rows, :], w_v[...], preferred_element_type=jnp.float32)
        return carry

    lax.fori_loop(0, NODES // 256, gather, 0)

    def finish(f, cols):
        at = (f + 2) % 3
        arrived = in_b[f].astype(jnp.bfloat16)

        def body(i, carry):
            rows = pl.ds(pl.multiple_of(i * 256, 256), 256)
            got = jnp.dot(r_v[rows, :], arrived, preferred_element_type=jnp.float32)
            got = got + acc_v[rows, cols : cols + 128]
            field = prog_v[at, rows, :].astype(jnp.float32)
            out_ref[at, rows, :] = (field + got * inv_v[rows, :]).astype(jnp.bfloat16)
            return carry

        lax.fori_loop(0, NODES // 256, body, 0)

    for g in GROUPS:
        remote(0, g).wait_recv()
    lane = lane_iota((1, 128))
    low = lane_iota((128, 128)) < 64
    blocks = []
    for chunk in range(2):
        row = jnp.zeros((1, 128), jnp.float32)
        for _, _, count, first in GROUPS:
            if first // 128 == chunk:
                at = first % 128
                row = jnp.where(
                    (lane >= at) & (lane < at + count), in_b[0, first + count : first + count + 1, :], row
                )
        col = jnp.transpose(jnp.broadcast_to(row, (128, 128)))
        high = col.astype(jnp.bfloat16).astype(jnp.float32)
        blocks.append(jnp.where(low, high, col - high).astype(jnp.bfloat16))
    arrived = jnp.concatenate(blocks, axis=0)

    def weights(i, carry):
        rows = pl.ds(pl.multiple_of(i * 256, 256), 256)
        w = jnp.dot(r_v[rows, :], arrived, preferred_element_type=jnp.float32)
        w = w + acc_v[rows, 128:256]
        w = w + pltpu.roll(w, 64, 1)
        inv_v[rows, :] = STEP_SIZE / w
        return carry

    lax.fori_loop(0, NODES // 256, weights, 0)
    finish(0, 0)
    for f in (1, 2):
        for g in GROUPS:
            remote(f, g).wait_recv()
        finish(f, 128 + 128 * f)
    for f in range(3):
        for g in GROUPS:
            remote(f, g).wait_send()


def solution(mesh):
    sizes = (mesh.shape["face"], mesh.shape["sub"])

    def local(prognostic, metric, coriolis, node_point, send_point, recv_point):
        result = pl.pallas_call(
            functools.partial(kernel, sizes),
            out_shape=pltpu.VMEM((3, NODES, LEV), jnp.bfloat16),
            in_specs=[pl.BlockSpec(memory_space=pltpu.HBM)] * 6,
            out_specs=pl.BlockSpec(memory_space=pltpu.VMEM),
            scratch_shapes=[
                pltpu.VMEM((3, NODES, LEV), jnp.bfloat16),
                pltpu.VMEM((4, 16, ELEMS), jnp.float32),
                pltpu.VMEM((16, ELEMS), jnp.float32),
                pltpu.VMEM((16, ELEMS), jnp.int32),
                pltpu.VMEM((1, LINKS), jnp.int32),
                pltpu.VMEM((1, LINKS), jnp.int32),
                pltpu.VMEM((3 * NODES, LEV), jnp.float32),
                pltpu.VMEM((ELEMS, 128), jnp.float32),
                pltpu.VMEM((5, NODES, LEV), jnp.float32),
                pltpu.VMEM((NODES, 512), jnp.bfloat16),
                pltpu.VMEM((ROWS, NODES), jnp.bfloat16),
                pltpu.VMEM((NODES, NODES), jnp.bfloat16),
                pltpu.VMEM((NODES, ROWS), jnp.bfloat16),
                pltpu.VMEM((NODES, 512), jnp.float32),
                pltpu.VMEM((NODES, LEV), jnp.float32),
                pltpu.VMEM((16, LEV), jnp.int32),
                pltpu.VMEM((3, ROWS, LEV), jnp.float32),
                pltpu.VMEM((3, ROWS, LEV), jnp.float32),
                pltpu.SemaphoreType.DMA((5 + 3 * BLOCKS,)),
                pltpu.SemaphoreType.DMA((3, 8)),
                pltpu.SemaphoreType.DMA((3, 8)),
            ],
            compiler_params=pltpu.CompilerParams(
                collective_id=0, has_side_effects=True, vmem_limit_bytes=40 * 1024 * 1024
            ),
        )(
            pltpu.with_memory_space_constraint(prognostic.reshape(3, NODES, LEV), pltpu.HBM),
            pltpu.with_memory_space_constraint(jnp.transpose(metric, (0, 2, 1)), pltpu.HBM),
            pltpu.with_memory_space_constraint(jnp.transpose(coriolis), pltpu.HBM),
            pltpu.with_memory_space_constraint(jnp.transpose(node_point), pltpu.HBM),
            pltpu.with_memory_space_constraint(send_point.reshape(1, LINKS), pltpu.HBM),
            pltpu.with_memory_space_constraint(recv_point.reshape(1, LINKS), pltpu.HBM),
        )
        return result.reshape(3, ELEMS, 16, LEV)

    placed = (
        P(None, ("face", "sub"), None, None),
        P(None, ("face", "sub"), None),
        P(("face", "sub"), None),
        P(("face", "sub"), None),
        P(("face", "sub")),
        P(("face", "sub")),
    )
    return jax.shard_map(
        local,
        mesh=mesh,
        in_specs=placed,
        out_specs=P(None, ("face", "sub"), None, None),
        check_vma=False,
    )
```

```python
import functools
import math

import jax
import jax.numpy as jnp
import numpy as np
from jax import lax
from jax.experimental import pallas as pl
from jax.experimental.pallas import tpu as pltpu
from jax.sharding import PartitionSpec as P

MESH = pl.DeviceIdType.MESH
BX = 32
BY = 2
ELEMS = BX * BY
NODES = ELEMS * 16
LEV = 128
SIDE = 3 * BY + 1
TOP = 3 * BX + 1
LINKS = 2 * SIDE + 2 * TOP + 4
STEP_SIZE = 0.1
BLK = 16
BLOCKS = ELEMS // BLK
BROWS = 16 * BLK

GROUPS = (
    (2, 2 * SIDE, TOP, 0),
    (3, 2 * SIDE + TOP, TOP, 128),
    (0, 0, SIDE, 104),
    (1, SIDE, SIDE, 232),
    (4, 2 * SIDE + 2 * TOP, 1, 112),
    (5, 2 * SIDE + 2 * TOP + 1, 1, 240),
    (6, 2 * SIDE + 2 * TOP + 2, 1, 120),
    (7, 2 * SIDE + 2 * TOP + 3, 1, 248),
)
ROWS = 256


def gll_tables():
    abscissa = np.array([-1.0, -math.sqrt(0.2), math.sqrt(0.2), 1.0])
    legendre = 0.5 * (5.0 * abscissa * abscissa * abscissa - 3.0 * abscissa)
    derivative = np.zeros((4, 4))
    for target in range(4):
        for source in range(4):
            if target != source:
                derivative[target, source] = legendre[target] / (
                    legendre[source] * (abscissa[target] - abscissa[source])
                )
    derivative[0, 0] = -3.0
    derivative[3, 3] = 3.0
    weights = np.array([1.0, 5.0, 5.0, 1.0]) / 6.0
    return derivative, weights


DERIV, GLL = gll_tables()
EV0 = float(0.5 * (DERIV[0, 0] + DERIV[0, 3]))
EV1 = float(0.5 * (DERIV[1, 0] + DERIV[1, 3]))
OD00 = float(0.5 * (DERIV[0, 0] - DERIV[0, 3]))
OD01 = float(0.5 * (DERIV[0, 1] - DERIV[0, 2]))
OD10 = float(0.5 * (DERIV[1, 0] - DERIV[1, 3]))
OD11 = float(0.5 * (DERIV[1, 1] - DERIV[1, 2]))


def derive4(s):
    o0 = s[0] - s[3]
    o1 = s[1] - s[2]
    q = (s[0] + s[3]) - (s[1] + s[2])
    h0 = OD00 * o0 + OD01 * o1
    h1 = OD10 * o0 + OD11 * o1
    g0 = EV0 * q
    g1 = EV1 * q
    return [h0 + g0, h1 + g1, h1 - g1, h0 - g0]


def along_cols(s):
    out = []
    for r in range(4):
        out += derive4(s[4 * r : 4 * r + 4])
    return out


def along_rows(s):
    out = [None] * 16
    for c in range(4):
        for r, value in enumerate(derive4(s[c::4])):
            out[4 * r + c] = value
    return out


NODE_W = [float(GLL[n // 4] * GLL[n % 4]) for n in range(16)]


def lane_iota(shape):
    return lax.broadcasted_iota(jnp.int32, shape, len(shape) - 1)


def padded_slots(ref):
    x = jnp.concatenate(
        [jnp.broadcast_to(ref[...], (8, LINKS)), jnp.full((8, ROWS - LINKS), -1, jnp.int32)], axis=1
    )
    lane = lane_iota((8, ROWS))
    out = jnp.full((8, ROWS), -1, jnp.int32)
    for _, first, count, row in GROUPS:
        moved = pltpu.roll(x, (row - first) % ROWS, 1)
        out = jnp.where((lane >= row) & (lane < row + count), moved, out)
    return out


def one_hot(col, row):
    return jnp.where(col == row, 1.0, 0.0).astype(jnp.bfloat16)


def kernel(
    sizes,
    prog_hbm, met_hbm, cor_hbm, np_hbm, sp_hbm, rp_hbm,
    out_ref,
    prog_v, met_v, cor_v, np_v, sp_v, rp_v,
    f_v, turn_v, ct_v, co_v, w_v, s_v, a_v, r_v, acc_v, inv_v, ids_v, out_b, in_b, out_w, in_w,
    in_sem, send_sem, recv_sem,
):
    n_face, n_sub = sizes
    total = n_face * n_sub
    lap = 4 * n_sub
    offsets = (1, -1, lap, -lap, lap + 1, -lap - 1, lap - 1, 1 - lap)
    me = lax.axis_index("face") * n_sub + lax.axis_index("sub")

    def device(offset):
        t = lax.rem(me + (offset + total), total)
        return (t // n_sub, lax.rem(t, n_sub))

    barrier = pltpu.get_barrier_semaphore()
    for offset in offsets:
        pl.semaphore_signal(barrier, inc=1, device_id=device(offset), device_id_type=MESH)
    loads = []
    for i, (src, dst) in enumerate(
        ((np_hbm, np_v), (sp_hbm, sp_v), (rp_hbm, rp_v), (met_hbm, met_v), (cor_hbm, cor_v))
    ):
        loads.append(pltpu.make_async_copy(src, dst, in_sem.at[i]))
    for f in range(3):
        loads.append(
            pltpu.make_async_copy(
                prog_hbm.at[f], prog_v.at[:, pl.ds(LEV * f, LEV)], in_sem.at[5 + f]
            )
        )
    for load in loads:
        load.start()

    def remote(f, g):
        group, _, count, row = g
        return pltpu.make_async_remote_copy(
            src_ref=out_b.at[f, pl.ds(row, count)],
            dst_ref=in_b.at[f, pl.ds(row, count)],
            send_sem=send_sem.at[f, group],
            recv_sem=recv_sem.at[f, group],
            device_id=device(offsets[group]),
            device_id_type=MESH,
        )

    def remote_weights(g):
        group, _, _, row = g
        return pltpu.make_async_remote_copy(
            src_ref=out_w.at[row // 128],
            dst_ref=in_w.at[group],
            send_sem=send_sem.at[3, group],
            recv_sem=recv_sem.at[3, group],
            device_id=device(offsets[group]),
            device_id_type=MESH,
        )

    edges = sorted((row, row + count) for _, _, count, row in GROUPS)
    for f in range(3):
        for (_, end), nxt in zip(edges, [e[0] for e in edges[1:]] + [ROWS]):
            in_b[f, end:nxt, :] = jnp.zeros((nxt - end, LEV), jnp.float32)

    for load in loads[:3]:
        load.wait()
    ids = np_v[...]
    ids2 = jnp.concatenate([ids, ids], axis=1)
    ids_v[...] = ids2
    rolled = [ids2 if i == 0 else pltpu.roll(ids2, 16 * i, 1) for i in range(4)]
    sub = lax.broadcasted_iota(jnp.int32, (8, LEV), 0)
    own = sub == lane_iota((8, LEV)) // BLK
    id_rows = []
    for k in range(BLOCKS):
        for h in range(2):
            pick = rolled[(-k) % 4][8 * h : 8 * h + 8]
            for i in range(1, 4):
                pick = jnp.where(sub % 4 == i, rolled[(i - k) % 4][8 * h : 8 * h + 8], pick)
            id_rows.append(jnp.sum(jnp.where(own, pick, 0), axis=0, keepdims=True))
    send_row = padded_slots(sp_v)
    recv_row = padded_slots(rp_v)
    for chunk in range(2):
        col = jnp.transpose(
            jnp.broadcast_to(send_row[0:1, 128 * chunk : 128 * chunk + 128], (128, 128))
        )
        for j in range(8):
            s_v[128 * chunk : 128 * chunk + 128, 128 * j : 128 * j + 128] = one_hot(col, id_rows[j])

    for load in loads[3:5]:
        load.wait()
    m_a, m_b, m_e, m_g = (met_v[i] for i in range(4))
    inverse = 1.0 / (m_a * m_g - m_b * m_e)
    node = lax.broadcasted_iota(jnp.int32, (16, ELEMS), 0)
    wr = jnp.where((node < 4) | (node >= 12), float(GLL[0]), float(GLL[1]))
    wc = jnp.where((node % 4 == 0) | (node % 4 == 3), float(GLL[0]), float(GLL[1]))
    mass = wr * wc * inverse
    coefs = jnp.concatenate(
        [m_a * inverse, m_b * inverse, m_e * inverse, m_g * inverse, mass * cor_v[...], mass, mass, mass],
        axis=0,
    )
    ct_v[...] = jnp.transpose(coefs)

    def rows_of(k, n):
        first = k * BROWS + n * BLK
        return pl.ds(first if isinstance(first, int) else pl.multiple_of(first, BLK), BLK)

    ct = ct_v[...]
    low = lane_iota((ELEMS, LEV)) < 64
    for n in range(16):
        for q in range(6):
            wide = jnp.broadcast_to(ct[:, q * 16 + n : q * 16 + n + 1], (ELEMS, LEV))
            if q == 5:
                high = wide.astype(jnp.bfloat16).astype(jnp.float32)
                wide = jnp.where(low, high, wide - high).astype(jnp.bfloat16)
            for k in range(BLOCKS):
                part = wide[BLK * k : BLK * k + BLK]
                if q == 5:
                    w_v[rows_of(k, n), 128:256] = part
                else:
                    co_v[q, rows_of(k, n), :] = part

    at = lax.broadcasted_iota(jnp.int32, (BROWS, BROWS), 0)
    turn_v[...] = one_hot(at % BLK * 16 + at // BLK, lane_iota((BROWS, BROWS)))

    for load in loads[5:]:
        load.wait()
    for k in range(BLOCKS):
        rows = slice(BROWS * k, BROWS * k + BROWS)
        f_v[rows, :] = jnp.dot(turn_v[...], prog_v[rows, :], preferred_element_type=jnp.float32)

    def fields_of(k):
        return [
            [f_v[rows_of(k, n), LEV * f : LEV * f + LEV] for n in range(16)] for f in range(3)
        ]

    for k in range(BLOCKS):
        u1, u2, phi = fields_of(k)
        con1, con2 = [], []
        for n in range(16):
            f1 = phi[n] * u1[n]
            f2 = phi[n] * u2[n]
            con1.append(co_v[0, rows_of(k, n), :] * f1 + co_v[1, rows_of(k, n), :] * f2)
            con2.append(co_v[2, rows_of(k, n), :] * f1 + co_v[3, rows_of(k, n), :] * f2)
        d1 = along_cols(con1)
        d2 = along_rows(con2)
        for n in range(16):
            w_v[rows_of(k, n), 0:128] = (-NODE_W[n] * (d1[n] + d2[n])).astype(jnp.bfloat16)
    sent = jnp.dot(s_v[...], w_v[:, 0:256], preferred_element_type=jnp.float32)
    out_b[0] = sent[:, 0:128]
    pl.semaphore_wait(barrier, len(offsets))
    for g in GROUPS:
        remote(0, g).start()

    weight = sent[:, 128:256]
    weight = weight + pltpu.roll(weight, 64, 1)
    diagonal = lax.broadcasted_iota(jnp.int32, (128, 128), 0) == lane_iota((128, 128))
    for chunk in range(2):
        out_w[chunk] = jnp.sum(
            jnp.where(diagonal, weight[128 * chunk : 128 * chunk + 128], 0.0), axis=0, keepdims=True
        )
    for g in GROUPS:
        remote_weights(g).start()

    def second_pass(k, carry):
        u1, u2, phi = fields_of(k)
        energy, cov1, cov2 = [], [], []
        for n in range(16):
            rows = rows_of(k, n)
            energy.append(0.5 * (u1[n] * u1[n] + u2[n] * u2[n]) + phi[n])
            cov1.append(co_v[3, rows, :] * u1[n] - co_v[2, rows, :] * u2[n])
            cov2.append(co_v[0, rows, :] * u2[n] - co_v[1, rows, :] * u1[n])
        curl1 = along_cols(cov2)
        curl2 = along_rows(cov1)
        e1 = along_cols(energy)
        e2 = along_rows(energy)
        for n in range(16):
            rows = rows_of(k, n)
            eta = NODE_W[n] * (curl1[n] - curl2[n]) + co_v[4, rows, :]
            grad1 = co_v[0, rows, :] * e1[n] + co_v[2, rows, :] * e2[n]
            grad2 = co_v[1, rows, :] * e1[n] + co_v[3, rows, :] * e2[n]
            w_v[rows, 256:384] = (eta * u2[n] - NODE_W[n] * grad1).astype(jnp.bfloat16)
            w_v[rows, 384:512] = (-eta * u1[n] - NODE_W[n] * grad2).astype(jnp.bfloat16)
        return carry

    lax.fori_loop(0, BLOCKS, second_pass, 0)
    sent = jnp.dot(s_v[...], w_v[:, 256:512], preferred_element_type=jnp.float32)
    for f in (1, 2):
        out_b[f] = sent[:, 128 * (f - 1) : 128 * f]

    face = lax.axis_index("face")
    turn = lax.rem(face // 2, 2) * 2 + 1 - lax.rem(face, 2)

    def send_wind():
        for f in (1, 2):
            for g in GROUPS:
                remote(f, g).start()

    pl.when(turn == 0)(send_wind)

    def table(i, carry):
        x = pltpu.roll(ids_v[...], LEV - 8 * i, 1)
        for lane in range(8):
            col = jnp.broadcast_to(x[:, lane : lane + 1], (16, LEV))
            rows = pl.ds(pl.multiple_of(i * 128 + lane * 16, 16), 16)
            for j in range(8):
                a_v[rows, 128 * j : 128 * j + 128] = one_hot(col, id_rows[j])
            for chunk in range(2):
                r_v[rows, 128 * chunk : 128 * chunk + 128] = one_hot(
                    col, recv_row[0:1, 128 * chunk : 128 * chunk + 128]
                )
        return carry

    lax.fori_loop(0, ELEMS // 8, table, 0)
    pl.when((turn == 1) | (turn == 2))(send_wind)

    def gather(i, carry):
        rows = pl.ds(pl.multiple_of(i * 256, 256), 256)
        acc_v[rows, :] = jnp.dot(a_v[rows, :], w_v[...], preferred_element_type=jnp.float32)
        return carry

    lax.fori_loop(0, NODES // 256, gather, 0)
    pl.when(turn == 3)(send_wind)

    def finish(f, cols):
        at = (f + 2) % 3
        got = jnp.dot(
            r_v[...], in_b[f].astype(jnp.bfloat16), preferred_element_type=jnp.float32
        )
        got = (got + acc_v[:, cols : cols + 128]) * inv_v[...]
        field = prog_v[:, LEV * at : LEV * at + LEV].astype(jnp.float32)
        out_ref[at] = (field + got).astype(jnp.bfloat16)

    for g in GROUPS:
        remote_weights(g).wait_recv()
    lane = lane_iota((1, 128))
    low = lane_iota((128, 128)) < 64
    blocks = []
    for chunk in range(2):
        row = jnp.zeros((1, 128), jnp.float32)
        for group, _, count, first in GROUPS:
            if first // 128 == chunk:
                at = first % 128
                row = jnp.where((lane >= at) & (lane < at + count), in_w[group], row)
        col = jnp.transpose(jnp.broadcast_to(row, (128, 128)))
        high = col.astype(jnp.bfloat16).astype(jnp.float32)
        blocks.append(jnp.where(low, high, col - high).astype(jnp.bfloat16))
    arrived = jnp.concatenate(blocks, axis=0)

    weight = jnp.dot(r_v[...], arrived, preferred_element_type=jnp.float32) + acc_v[:, 128:256]
    inv_v[...] = STEP_SIZE / (weight + pltpu.roll(weight, 64, 1))
    for f in range(3):
        for g in GROUPS:
            remote(f, g).wait_recv()
        finish(f, 128 * f + 128 if f else 0)
    for g in GROUPS:
        for f in range(3):
            remote(f, g).wait_send()
        remote_weights(g).wait_send()


def solution(mesh):
    sizes = (mesh.shape["face"], mesh.shape["sub"])

    def local(prognostic, metric, coriolis, node_point, send_point, recv_point):
        result = pl.pallas_call(
            functools.partial(kernel, sizes),
            out_shape=pltpu.VMEM((3, NODES, LEV), jnp.bfloat16),
            in_specs=[pl.BlockSpec(memory_space=pltpu.HBM)] * 6,
            out_specs=pl.BlockSpec(memory_space=pltpu.VMEM),
            scratch_shapes=[
                pltpu.VMEM((NODES, 3 * LEV), jnp.bfloat16),
                pltpu.VMEM((4, 16, ELEMS), jnp.float32),
                pltpu.VMEM((16, ELEMS), jnp.float32),
                pltpu.VMEM((16, ELEMS), jnp.int32),
                pltpu.VMEM((1, LINKS), jnp.int32),
                pltpu.VMEM((1, LINKS), jnp.int32),
                pltpu.VMEM((NODES, 3 * LEV), jnp.float32),
                pltpu.VMEM((BROWS, BROWS), jnp.bfloat16),
                pltpu.VMEM((ELEMS, 128), jnp.float32),
                pltpu.VMEM((5, NODES, LEV), jnp.float32),
                pltpu.VMEM((NODES, 512), jnp.bfloat16),
                pltpu.VMEM((ROWS, NODES), jnp.bfloat16),
                pltpu.VMEM((NODES, NODES), jnp.bfloat16),
                pltpu.VMEM((NODES, ROWS), jnp.bfloat16),
                pltpu.VMEM((NODES, 512), jnp.float32),
                pltpu.VMEM((NODES, LEV), jnp.float32),
                pltpu.VMEM((16, LEV), jnp.int32),
                pltpu.VMEM((3, ROWS, LEV), jnp.float32),
                pltpu.VMEM((3, ROWS, LEV), jnp.float32),
                pltpu.VMEM((2, 1, LEV), jnp.float32),
                pltpu.VMEM((8, 1, LEV), jnp.float32),
                pltpu.SemaphoreType.DMA((8,)),
                pltpu.SemaphoreType.DMA((4, 8)),
                pltpu.SemaphoreType.DMA((4, 8)),
            ],
            compiler_params=pltpu.CompilerParams(
                collective_id=0, has_side_effects=True, vmem_limit_bytes=40 * 1024 * 1024
            ),
        )(
            pltpu.with_memory_space_constraint(prognostic.reshape(3, NODES, LEV), pltpu.HBM),
            pltpu.with_memory_space_constraint(jnp.transpose(metric, (0, 2, 1)), pltpu.HBM),
            pltpu.with_memory_space_constraint(jnp.transpose(coriolis), pltpu.HBM),
            pltpu.with_memory_space_constraint(jnp.transpose(node_point), pltpu.HBM),
            pltpu.with_memory_space_constraint(send_point.reshape(1, LINKS), pltpu.HBM),
            pltpu.with_memory_space_constraint(recv_point.reshape(1, LINKS), pltpu.HBM),
        )
        return result.reshape(3, ELEMS, 16, LEV)

    placed = (
        P(None, ("face", "sub"), None, None),
        P(None, ("face", "sub"), None),
        P(("face", "sub"), None),
        P(("face", "sub"), None),
        P(("face", "sub")),
        P(("face", "sub")),
    )
    return jax.shard_map(
        local,
        mesh=mesh,
        in_specs=placed,
        out_specs=P(None, ("face", "sub"), None, None),
        check_vma=False,
    )
```

```python
import functools
import math

import jax
import jax.numpy as jnp
import numpy as np
from jax import lax
from jax.experimental import pallas as pl
from jax.experimental.pallas import tpu as pltpu
from jax.sharding import PartitionSpec as P

MESH = pl.DeviceIdType.MESH
BX = 32
BY = 2
ELEMS = BX * BY
NODES = ELEMS * 16
LEV = 128
SIDE = 3 * BY + 1
TOP = 3 * BX + 1
LINKS = 2 * SIDE + 2 * TOP + 4
STEP_SIZE = 0.1
BLK = 16
BLOCKS = ELEMS // BLK
PLANES = 16
BROWS = 16 * BLK

GROUPS = (
    (2, 2 * SIDE, TOP, 0),
    (3, 2 * SIDE + TOP, TOP, 128),
    (0, 0, SIDE, 104),
    (1, SIDE, SIDE, 232),
    (4, 2 * SIDE + 2 * TOP, 1, 112),
    (5, 2 * SIDE + 2 * TOP + 1, 1, 240),
    (6, 2 * SIDE + 2 * TOP + 2, 1, 120),
    (7, 2 * SIDE + 2 * TOP + 3, 1, 248),
)
ROWS = 256


def gll_tables():
    abscissa = np.array([-1.0, -math.sqrt(0.2), math.sqrt(0.2), 1.0])
    legendre = 0.5 * (5.0 * abscissa * abscissa * abscissa - 3.0 * abscissa)
    derivative = np.zeros((4, 4))
    for target in range(4):
        for source in range(4):
            if target != source:
                derivative[target, source] = legendre[target] / (
                    legendre[source] * (abscissa[target] - abscissa[source])
                )
    derivative[0, 0] = -3.0
    derivative[3, 3] = 3.0
    weights = np.array([1.0, 5.0, 5.0, 1.0]) / 6.0
    return derivative, weights


DERIV, GLL = gll_tables()
EV0 = float(0.5 * (DERIV[0, 0] + DERIV[0, 3]))
EV1 = float(0.5 * (DERIV[1, 0] + DERIV[1, 3]))
OD00 = float(0.5 * (DERIV[0, 0] - DERIV[0, 3]))
OD01 = float(0.5 * (DERIV[0, 1] - DERIV[0, 2]))
OD10 = float(0.5 * (DERIV[1, 0] - DERIV[1, 3]))
OD11 = float(0.5 * (DERIV[1, 1] - DERIV[1, 2]))


def derive4(s):
    o0 = s[0] - s[3]
    o1 = s[1] - s[2]
    q = (s[0] + s[3]) - (s[1] + s[2])
    h0 = OD00 * o0 + OD01 * o1
    h1 = OD10 * o0 + OD11 * o1
    g0 = EV0 * q
    g1 = EV1 * q
    return [h0 + g0, h1 + g1, h1 - g1, h0 - g0]


def along_cols(s):
    out = []
    for r in range(4):
        out += derive4(s[4 * r : 4 * r + 4])
    return out


def along_rows(s):
    out = [None] * 16
    for c in range(4):
        for r, value in enumerate(derive4(s[c::4])):
            out[4 * r + c] = value
    return out


NODE_W = [float(GLL[n // 4] * GLL[n % 4]) for n in range(16)]


def lane_iota(shape):
    return lax.broadcasted_iota(jnp.int32, shape, len(shape) - 1)


def padded_slots(ref):
    x = jnp.concatenate(
        [jnp.broadcast_to(ref[...], (8, LINKS)), jnp.full((8, ROWS - LINKS), -1, jnp.int32)], axis=1
    )
    lane = lane_iota((8, ROWS))
    out = jnp.full((8, ROWS), -1, jnp.int32)
    for _, first, count, row in GROUPS:
        moved = pltpu.roll(x, (row - first) % ROWS, 1)
        out = jnp.where((lane >= row) & (lane < row + count), moved, out)
    return out


def one_hot(col, row):
    return jnp.where(col == row, 1.0, 0.0).astype(jnp.bfloat16)


def kernel(
    sizes,
    prog_hbm, met_hbm, cor_hbm, np_hbm, sp_hbm, rp_hbm,
    out_ref,
    prog_v, met_v, cor_v, np_v, sp_v, rp_v,
    f_v, turn_v, ct_v, co_v, w_v, s_v, a_v, r_v, acc_v, inv_v, ids_v, out_b, in_b, out_w, in_w,
    in_sem, send_sem, recv_sem,
):
    n_face, n_sub = sizes
    total = n_face * n_sub
    lap = 4 * n_sub
    offsets = (1, -1, lap, -lap, lap + 1, -lap - 1, lap - 1, 1 - lap)
    me = lax.axis_index("face") * n_sub + lax.axis_index("sub")

    def device(offset):
        t = lax.rem(me + (offset + total), total)
        return (t // n_sub, lax.rem(t, n_sub))

    barrier = pltpu.get_barrier_semaphore()
    for offset in offsets:
        pl.semaphore_signal(barrier, inc=1, device_id=device(offset), device_id_type=MESH)
    loads = []
    for i, (src, dst) in enumerate(
        ((np_hbm, np_v), (sp_hbm, sp_v), (rp_hbm, rp_v), (met_hbm, met_v), (cor_hbm, cor_v))
    ):
        loads.append(pltpu.make_async_copy(src, dst, in_sem.at[i]))
    for f in range(3):
        loads.append(
            pltpu.make_async_copy(
                prog_hbm.at[f], prog_v.at[:, pl.ds(LEV * f, LEV)], in_sem.at[5 + f]
            )
        )
    for load in loads:
        load.start()

    def remote(f, g):
        group, _, count, row = g
        return pltpu.make_async_remote_copy(
            src_ref=out_b.at[f, pl.ds(row, count)],
            dst_ref=in_b.at[f, pl.ds(row, count)],
            send_sem=send_sem.at[f, group],
            recv_sem=recv_sem.at[f, group],
            device_id=device(offsets[group]),
            device_id_type=MESH,
        )

    def remote_weights(g):
        group, _, _, row = g
        return pltpu.make_async_remote_copy(
            src_ref=out_w.at[row // 128],
            dst_ref=in_w.at[group],
            send_sem=send_sem.at[3, group],
            recv_sem=recv_sem.at[3, group],
            device_id=device(offsets[group]),
            device_id_type=MESH,
        )

    edges = sorted((row, row + count) for _, _, count, row in GROUPS)
    for f in range(3):
        for (_, end), nxt in zip(edges, [e[0] for e in edges[1:]] + [ROWS]):
            in_b[f, end:nxt, :] = jnp.zeros((nxt - end, LEV), jnp.float32)

    for load in loads[:3]:
        load.wait()
    ids = np_v[...]
    ids2 = jnp.concatenate([ids, ids], axis=1)
    ids_v[...] = ids2
    rolled = [ids2 if i == 0 else pltpu.roll(ids2, 16 * i, 1) for i in range(4)]
    sub = lax.broadcasted_iota(jnp.int32, (8, LEV), 0)
    own = sub == lane_iota((8, LEV)) // BLK
    id_rows = []
    for k in range(BLOCKS):
        for h in range(2):
            pick = rolled[(-k) % 4][8 * h : 8 * h + 8]
            for i in range(1, 4):
                pick = jnp.where(sub % 4 == i, rolled[(i - k) % 4][8 * h : 8 * h + 8], pick)
            id_rows.append(jnp.sum(jnp.where(own, pick, 0), axis=0, keepdims=True))
    send_row = padded_slots(sp_v)
    recv_row = padded_slots(rp_v)
    for chunk in range(2):
        col = jnp.transpose(
            jnp.broadcast_to(send_row[0:1, 128 * chunk : 128 * chunk + 128], (128, 128))
        )
        for j in range(8):
            s_v[128 * chunk : 128 * chunk + 128, 128 * j : 128 * j + 128] = one_hot(col, id_rows[j])

    for load in loads[3:5]:
        load.wait()
    m_a, m_b, m_e, m_g = (met_v[i] for i in range(4))
    inverse = 1.0 / (m_a * m_g - m_b * m_e)
    node = lax.broadcasted_iota(jnp.int32, (16, ELEMS), 0)
    wr = jnp.where((node < 4) | (node >= 12), float(GLL[0]), float(GLL[1]))
    wc = jnp.where((node % 4 == 0) | (node % 4 == 3), float(GLL[0]), float(GLL[1]))
    mass = wr * wc * inverse
    coefs = jnp.concatenate(
        [m_a * inverse, m_b * inverse, m_e * inverse, m_g * inverse, mass * cor_v[...], mass, mass, mass],
        axis=0,
    )
    ct_v[...] = jnp.transpose(coefs)

    def rows_of(k, n):
        first = k * BROWS + n * BLK
        return pl.ds(first if isinstance(first, int) else pl.multiple_of(first, BLK), BLK)

    ct = ct_v[...]
    low = lane_iota((ELEMS, LEV)) < 64
    for n in range(16):
        for q in range(6):
            wide = jnp.broadcast_to(ct[:, q * 16 + n : q * 16 + n + 1], (ELEMS, LEV))
            if q == 5:
                high = wide.astype(jnp.bfloat16).astype(jnp.float32)
                wide = jnp.where(low, high, wide - high).astype(jnp.bfloat16)
            for k in range(BLOCKS):
                part = wide[BLK * k : BLK * k + BLK]
                if q == 5:
                    w_v[rows_of(k, n), 128:256] = part
                else:
                    co_v[q, rows_of(k, n), :] = part

    at = lax.broadcasted_iota(jnp.int32, (BROWS, BROWS), 0)
    turn_v[...] = one_hot(at % BLK * 16 + at // BLK, lane_iota((BROWS, BROWS)))

    for load in loads[5:]:
        load.wait()
    for k in range(BLOCKS):
        rows = slice(BROWS * k, BROWS * k + BROWS)
        f_v[rows, :] = jnp.dot(turn_v[...], prog_v[rows, :], preferred_element_type=jnp.float32)

    def fields_of(k):
        return [
            [f_v[rows_of(k, n), LEV * f : LEV * f + LEV] for n in range(16)] for f in range(3)
        ]

    for k in range(BLOCKS):
        u1, u2, phi = fields_of(k)
        con1, con2 = [], []
        for n in range(16):
            f1 = phi[n] * u1[n]
            f2 = phi[n] * u2[n]
            con1.append(co_v[0, rows_of(k, n), :] * f1 + co_v[1, rows_of(k, n), :] * f2)
            con2.append(co_v[2, rows_of(k, n), :] * f1 + co_v[3, rows_of(k, n), :] * f2)
        d1 = along_cols(con1)
        d2 = along_rows(con2)
        for n in range(16):
            w_v[rows_of(k, n), 0:128] = (-NODE_W[n] * (d1[n] + d2[n])).astype(jnp.bfloat16)
    sent = jnp.dot(s_v[...], w_v[:, 0:256], preferred_element_type=jnp.float32)
    out_b[0] = sent[:, 0:128]
    def send(fields, groups):
        for f in fields:
            for g in groups:
                remote(f, g).start()

    def second_pass(k, carry):
        u1, u2, phi = fields_of(k)
        energy, cov1, cov2 = [], [], []
        for n in range(16):
            rows = rows_of(k, n)
            energy.append(0.5 * (u1[n] * u1[n] + u2[n] * u2[n]) + phi[n])
            cov1.append(co_v[3, rows, :] * u1[n] - co_v[2, rows, :] * u2[n])
            cov2.append(co_v[0, rows, :] * u2[n] - co_v[1, rows, :] * u1[n])
        curl1 = along_cols(cov2)
        curl2 = along_rows(cov1)
        e1 = along_cols(energy)
        e2 = along_rows(energy)
        for n in range(16):
            rows = rows_of(k, n)
            eta = NODE_W[n] * (curl1[n] - curl2[n]) + co_v[4, rows, :]
            grad1 = co_v[0, rows, :] * e1[n] + co_v[2, rows, :] * e2[n]
            grad2 = co_v[1, rows, :] * e1[n] + co_v[3, rows, :] * e2[n]
            w_v[rows, 256:384] = (eta * u2[n] - NODE_W[n] * grad1).astype(jnp.bfloat16)
            w_v[rows, 384:512] = (-eta * u1[n] - NODE_W[n] * grad2).astype(jnp.bfloat16)
        return carry

    def wind():
        lax.fori_loop(0, BLOCKS, second_pass, 0)
        sent = jnp.dot(s_v[...], w_v[:, 256:512], preferred_element_type=jnp.float32)
        for f in (1, 2):
            out_b[f] = sent[:, 128 * (f - 1) : 128 * f]

    def table(i, carry):
        x = pltpu.roll(ids_v[...], LEV - 8 * i, 1)
        for lane in range(8):
            col = jnp.broadcast_to(x[:, lane : lane + 1], (16, LEV))
            rows = pl.ds(pl.multiple_of(i * 128 + lane * 16, 16), 16)
            for j in range(8):
                a_v[rows, 128 * j : 128 * j + 128] = one_hot(col, id_rows[j])
            for chunk in range(2):
                r_v[rows, 128 * chunk : 128 * chunk + 128] = one_hot(
                    col, recv_row[0:1, 128 * chunk : 128 * chunk + 128]
                )
        return carry

    def tables():
        lax.fori_loop(0, ELEMS // 8, table, 0)

    def gather(i, carry):
        rows = pl.ds(pl.multiple_of(i * 256, 256), 256)
        acc_v[rows, :] = jnp.dot(a_v[rows, :], w_v[...], preferred_element_type=jnp.float32)
        return carry

    def sums():
        lax.fori_loop(0, NODES // 256, gather, 0)

    face = lax.axis_index("face")
    plane = lax.rem(face // 2, PLANES)
    first = plane < 4

    @pl.when(first)
    def _():
        wind()
        tables()
        sums()

    pl.semaphore_wait(barrier, len(offsets))
    send((0,), GROUPS)
    weight = sent[:, 128:256]
    weight = weight + pltpu.roll(weight, 64, 1)
    diagonal = lax.broadcasted_iota(jnp.int32, (128, 128), 0) == lane_iota((128, 128))
    for chunk in range(2):
        out_w[chunk] = jnp.sum(
            jnp.where(diagonal, weight[128 * chunk : 128 * chunk + 128], 0.0), axis=0, keepdims=True
        )
    for g in GROUPS:
        remote_weights(g).start()

    @pl.when(first)
    def _():
        send((1, 2), GROUPS)

    @pl.when(jnp.logical_not(first))
    def _():
        turn = lax.rem(plane, 2) * 2 + 1 - lax.rem(face, 2)
        wind()
        pl.when(turn == 0)(lambda: send((1, 2), GROUPS[:2]))
        send((1, 2), GROUPS[2:])
        tables()
        pl.when((turn == 1) | (turn == 2))(lambda: send((1, 2), GROUPS[:2]))
        sums()
        pl.when(turn == 3)(lambda: send((1, 2), GROUPS[:2]))

    def finish(f, cols):
        at = (f + 2) % 3
        got = jnp.dot(
            r_v[...], in_b[f].astype(jnp.bfloat16), preferred_element_type=jnp.float32
        )
        got = (got + acc_v[:, cols : cols + 128]) * inv_v[...]
        field = prog_v[:, LEV * at : LEV * at + LEV].astype(jnp.float32)
        out_ref[at] = (field + got).astype(jnp.bfloat16)

    for g in GROUPS:
        remote_weights(g).wait_recv()
    lane = lane_iota((1, 128))
    low = lane_iota((128, 128)) < 64
    blocks = []
    for chunk in range(2):
        row = jnp.zeros((1, 128), jnp.float32)
        for group, _, count, first in GROUPS:
            if first // 128 == chunk:
                at = first % 128
                row = jnp.where((lane >= at) & (lane < at + count), in_w[group], row)
        col = jnp.transpose(jnp.broadcast_to(row, (128, 128)))
        high = col.astype(jnp.bfloat16).astype(jnp.float32)
        blocks.append(jnp.where(low, high, col - high).astype(jnp.bfloat16))
    arrived = jnp.concatenate(blocks, axis=0)

    weight = jnp.dot(r_v[...], arrived, preferred_element_type=jnp.float32) + acc_v[:, 128:256]
    inv_v[...] = STEP_SIZE / (weight + pltpu.roll(weight, 64, 1))
    for f in range(3):
        for g in GROUPS:
            remote(f, g).wait_recv()
        finish(f, 128 * f + 128 if f else 0)
    for g in GROUPS:
        for f in range(3):
            remote(f, g).wait_send()
        remote_weights(g).wait_send()


def solution(mesh):
    sizes = (mesh.shape["face"], mesh.shape["sub"])

    def local(prognostic, metric, coriolis, node_point, send_point, recv_point):
        result = pl.pallas_call(
            functools.partial(kernel, sizes),
            out_shape=pltpu.VMEM((3, NODES, LEV), jnp.bfloat16),
            in_specs=[pl.BlockSpec(memory_space=pltpu.HBM)] * 6,
            out_specs=pl.BlockSpec(memory_space=pltpu.VMEM),
            scratch_shapes=[
                pltpu.VMEM((NODES, 3 * LEV), jnp.bfloat16),
                pltpu.VMEM((4, 16, ELEMS), jnp.float32),
                pltpu.VMEM((16, ELEMS), jnp.float32),
                pltpu.VMEM((16, ELEMS), jnp.int32),
                pltpu.VMEM((1, LINKS), jnp.int32),
                pltpu.VMEM((1, LINKS), jnp.int32),
                pltpu.VMEM((NODES, 3 * LEV), jnp.float32),
                pltpu.VMEM((BROWS, BROWS), jnp.bfloat16),
                pltpu.VMEM((ELEMS, 128), jnp.float32),
                pltpu.VMEM((5, NODES, LEV), jnp.float32),
                pltpu.VMEM((NODES, 512), jnp.bfloat16),
                pltpu.VMEM((ROWS, NODES), jnp.bfloat16),
                pltpu.VMEM((NODES, NODES), jnp.bfloat16),
                pltpu.VMEM((NODES, ROWS), jnp.bfloat16),
                pltpu.VMEM((NODES, 512), jnp.float32),
                pltpu.VMEM((NODES, LEV), jnp.float32),
                pltpu.VMEM((16, LEV), jnp.int32),
                pltpu.VMEM((3, ROWS, LEV), jnp.float32),
                pltpu.VMEM((3, ROWS, LEV), jnp.float32),
                pltpu.VMEM((2, 1, LEV), jnp.float32),
                pltpu.VMEM((8, 1, LEV), jnp.float32),
                pltpu.SemaphoreType.DMA((8,)),
                pltpu.SemaphoreType.DMA((4, 8)),
                pltpu.SemaphoreType.DMA((4, 8)),
            ],
            compiler_params=pltpu.CompilerParams(
                collective_id=0, has_side_effects=True, vmem_limit_bytes=40 * 1024 * 1024
            ),
        )(
            pltpu.with_memory_space_constraint(prognostic.reshape(3, NODES, LEV), pltpu.HBM),
            pltpu.with_memory_space_constraint(jnp.transpose(metric, (0, 2, 1)), pltpu.HBM),
            pltpu.with_memory_space_constraint(jnp.transpose(coriolis), pltpu.HBM),
            pltpu.with_memory_space_constraint(jnp.transpose(node_point), pltpu.HBM),
            pltpu.with_memory_space_constraint(send_point.reshape(1, LINKS), pltpu.HBM),
            pltpu.with_memory_space_constraint(recv_point.reshape(1, LINKS), pltpu.HBM),
        )
        return result.reshape(3, ELEMS, 16, LEV)

    placed = (
        P(None, ("face", "sub"), None, None),
        P(None, ("face", "sub"), None),
        P(("face", "sub"), None),
        P(("face", "sub"), None),
        P(("face", "sub")),
        P(("face", "sub")),
    )
    return jax.shard_map(
        local,
        mesh=mesh,
        in_specs=placed,
        out_specs=P(None, ("face", "sub"), None, None),
        check_vma=False,
    )
```

```python
import functools
import math

import jax
import jax.numpy as jnp
import numpy as np
from jax import lax
from jax.experimental import pallas as pl
from jax.experimental.pallas import tpu as pltpu
from jax.sharding import PartitionSpec as P

MESH = pl.DeviceIdType.MESH
BX = 32
BY = 2
ELEMS = BX * BY
NODES = ELEMS * 16
LEV = 128
SIDE = 3 * BY + 1
TOP = 3 * BX + 1
LINKS = 2 * SIDE + 2 * TOP + 4
STEP_SIZE = 0.1
BLK = 16
BLOCKS = ELEMS // BLK
HALF = NODES // 2
MASS = 5
PLANES = 16
BROWS = 16 * BLK

GROUPS = (
    (2, 2 * SIDE, TOP, 0),
    (3, 2 * SIDE + TOP, TOP, 128),
    (0, 0, SIDE, 104),
    (1, SIDE, SIDE, 232),
    (4, 2 * SIDE + 2 * TOP, 1, 112),
    (5, 2 * SIDE + 2 * TOP + 1, 1, 240),
    (6, 2 * SIDE + 2 * TOP + 2, 1, 120),
    (7, 2 * SIDE + 2 * TOP + 3, 1, 248),
)
ROWS = 256


def gll_tables():
    abscissa = np.array([-1.0, -math.sqrt(0.2), math.sqrt(0.2), 1.0])
    legendre = 0.5 * (5.0 * abscissa * abscissa * abscissa - 3.0 * abscissa)
    derivative = np.zeros((4, 4))
    for target in range(4):
        for source in range(4):
            if target != source:
                derivative[target, source] = legendre[target] / (
                    legendre[source] * (abscissa[target] - abscissa[source])
                )
    derivative[0, 0] = -3.0
    derivative[3, 3] = 3.0
    weights = np.array([1.0, 5.0, 5.0, 1.0]) / 6.0
    return derivative, weights


DERIV, GLL = gll_tables()
EV0 = float(0.5 * (DERIV[0, 0] + DERIV[0, 3]))
EV1 = float(0.5 * (DERIV[1, 0] + DERIV[1, 3]))
OD00 = float(0.5 * (DERIV[0, 0] - DERIV[0, 3]))
OD01 = float(0.5 * (DERIV[0, 1] - DERIV[0, 2]))
OD10 = float(0.5 * (DERIV[1, 0] - DERIV[1, 3]))
OD11 = float(0.5 * (DERIV[1, 1] - DERIV[1, 2]))


def derive4(s):
    o0 = s[0] - s[3]
    o1 = s[1] - s[2]
    q = (s[0] + s[3]) - (s[1] + s[2])
    h0 = OD00 * o0 + OD01 * o1
    h1 = OD10 * o0 + OD11 * o1
    g0 = EV0 * q
    g1 = EV1 * q
    return [h0 + g0, h1 + g1, h1 - g1, h0 - g0]


def along_cols(s):
    out = []
    for r in range(4):
        out += derive4(s[4 * r : 4 * r + 4])
    return out


def along_rows(s):
    out = [None] * 16
    for c in range(4):
        for r, value in enumerate(derive4(s[c::4])):
            out[4 * r + c] = value
    return out


NODE_W = [float(GLL[n // 4] * GLL[n % 4]) for n in range(16)]


def lane_iota(shape):
    return lax.broadcasted_iota(jnp.int32, shape, len(shape) - 1)


def padded_slots(ref):
    x = jnp.concatenate(
        [jnp.broadcast_to(ref[...], (8, LINKS)), jnp.full((8, ROWS - LINKS), -1, jnp.int32)], axis=1
    )
    lane = lane_iota((8, ROWS))
    out = jnp.full((8, ROWS), -1, jnp.int32)
    for _, first, count, row in GROUPS:
        moved = pltpu.roll(x, (row - first) % ROWS, 1)
        out = jnp.where((lane >= row) & (lane < row + count), moved, out)
    return out


def one_hot(col, row):
    return jnp.where(col == row, 1.0, 0.0).astype(jnp.bfloat16)


def kernel(
    sizes,
    prog_hbm, met_hbm, cor_hbm, np_hbm, sp_hbm, rp_hbm,
    out_ref,
    prog_v, met_v, cor_v, np_v, sp_v, rp_v,
    f_v, turn_v, ct_v, co_v, w_v, s_v, a_v, r_v, acc_v, inv_v, ids_v, out_b, in_b, out_w, in_w,
    in_sem, send_sem, recv_sem,
):
    n_face, n_sub = sizes
    total = n_face * n_sub
    lap = 4 * n_sub
    offsets = (1, -1, lap, -lap, lap + 1, -lap - 1, lap - 1, 1 - lap)
    me = lax.axis_index("face") * n_sub + lax.axis_index("sub")

    def device(offset):
        t = lax.rem(me + (offset + total), total)
        return (t // n_sub, lax.rem(t, n_sub))

    barrier = pltpu.get_barrier_semaphore()
    for offset in offsets:
        pl.semaphore_signal(barrier, inc=1, device_id=device(offset), device_id_type=MESH)
    loads = []
    for i, (src, dst) in enumerate(
        ((np_hbm, np_v), (sp_hbm, sp_v), (rp_hbm, rp_v), (met_hbm, met_v), (cor_hbm, cor_v))
    ):
        loads.append(pltpu.make_async_copy(src, dst, in_sem.at[i]))
    for h in range(2):
        rows = pl.ds(HALF * h, HALF)
        for f in range(3):
            loads.append(
                pltpu.make_async_copy(
                    prog_hbm.at[f, rows], prog_v.at[f, rows], in_sem.at[5 + 3 * h + f]
                )
            )
    for load in loads:
        load.start()

    def remote(f, g):
        group, _, count, row = g
        return pltpu.make_async_remote_copy(
            src_ref=out_b.at[f, pl.ds(row, count)],
            dst_ref=in_b.at[f, pl.ds(row, count)],
            send_sem=send_sem.at[f, group],
            recv_sem=recv_sem.at[f, group],
            device_id=device(offsets[group]),
            device_id_type=MESH,
        )

    def remote_weights(g):
        group, _, _, row = g
        return pltpu.make_async_remote_copy(
            src_ref=out_w.at[row // 128],
            dst_ref=in_w.at[group],
            send_sem=send_sem.at[3, group],
            recv_sem=recv_sem.at[3, group],
            device_id=device(offsets[group]),
            device_id_type=MESH,
        )

    edges = sorted((row, row + count) for _, _, count, row in GROUPS)
    for f in range(3):
        for (_, end), nxt in zip(edges, [e[0] for e in edges[1:]] + [ROWS]):
            in_b[f, end:nxt, :] = jnp.zeros((nxt - end, LEV), jnp.float32)

    for load in loads[:3]:
        load.wait()
    ids = np_v[...]
    ids2 = jnp.concatenate([ids, ids], axis=1)
    ids_v[...] = ids2
    rolled = [ids2 if i == 0 else pltpu.roll(ids2, 16 * i, 1) for i in range(4)]
    sub = lax.broadcasted_iota(jnp.int32, (8, LEV), 0)
    own = sub == lane_iota((8, LEV)) // BLK
    id_rows = []
    for k in range(BLOCKS):
        for h in range(2):
            pick = rolled[(-k) % 4][8 * h : 8 * h + 8]
            for i in range(1, 4):
                pick = jnp.where(sub % 4 == i, rolled[(i - k) % 4][8 * h : 8 * h + 8], pick)
            id_rows.append(jnp.sum(jnp.where(own, pick, 0), axis=0, keepdims=True))
    send_row = padded_slots(sp_v)
    recv_row = padded_slots(rp_v)
    for chunk in range(2):
        col = jnp.transpose(
            jnp.broadcast_to(send_row[0:1, 128 * chunk : 128 * chunk + 128], (128, 128))
        )
        for j in range(8):
            s_v[128 * chunk : 128 * chunk + 128, 128 * j : 128 * j + 128] = one_hot(col, id_rows[j])

    for load in loads[3:5]:
        load.wait()
    m_a, m_b, m_e, m_g = (met_v[i] for i in range(4))
    inverse = 1.0 / (m_a * m_g - m_b * m_e)
    node = lax.broadcasted_iota(jnp.int32, (16, ELEMS), 0)
    wr = jnp.where((node < 4) | (node >= 12), float(GLL[0]), float(GLL[1]))
    wc = jnp.where((node % 4 == 0) | (node % 4 == 3), float(GLL[0]), float(GLL[1]))
    mass = wr * wc * inverse
    coefs = jnp.concatenate(
        [m_a * inverse, m_b * inverse, m_e * inverse, m_g * inverse, mass * cor_v[...], mass, mass, mass],
        axis=0,
    )
    ct_v[...] = jnp.transpose(coefs)

    def rows_of(k, n):
        first = k * BROWS + n * BLK
        return pl.ds(first if isinstance(first, int) else pl.multiple_of(first, BLK), BLK)

    at = lax.broadcasted_iota(jnp.int32, (BROWS, BROWS), 0)
    turn_v[...] = one_hot(at % BLK * 16 + at // BLK, lane_iota((BROWS, BROWS)))

    def spread(q):
        for n in range(16):
            wide = jnp.broadcast_to(ct_v[:, q * 16 + n : q * 16 + n + 1], (ELEMS, LEV))
            if q == MASS:
                high = wide.astype(jnp.bfloat16).astype(jnp.float32)
                low = lane_iota((ELEMS, LEV)) >= 64
                wide = jnp.where(low, wide - high, high).astype(jnp.bfloat16)
            for k in range(BLOCKS):
                part = wide[BLK * k : BLK * k + BLK]
                if q == MASS:
                    w_v[rows_of(k, n), 128:256] = part
                else:
                    co_v[q, rows_of(k, n), :] = part

    def turn_half(h):
        for load in loads[5 + 3 * h : 8 + 3 * h]:
            load.wait()
        for k in (2 * h, 2 * h + 1):
            rows = slice(BROWS * k, BROWS * k + BROWS)
            block = jnp.concatenate([prog_v[f, rows] for f in range(3)], axis=1)
            f_v[rows, :] = jnp.dot(turn_v[...], block, preferred_element_type=jnp.float32)

    spread(0)
    spread(1)
    turn_half(0)
    spread(2)
    spread(3)
    spread(MASS)
    turn_half(1)

    def fields_of(k):
        return [
            [f_v[rows_of(k, n), LEV * f : LEV * f + LEV] for n in range(16)] for f in range(3)
        ]

    for k in range(BLOCKS):
        u1, u2, phi = fields_of(k)
        con1, con2 = [], []
        for n in range(16):
            f1 = phi[n] * u1[n]
            f2 = phi[n] * u2[n]
            con1.append(co_v[0, rows_of(k, n), :] * f1 + co_v[1, rows_of(k, n), :] * f2)
            con2.append(co_v[2, rows_of(k, n), :] * f1 + co_v[3, rows_of(k, n), :] * f2)
        d1 = along_cols(con1)
        d2 = along_rows(con2)
        for n in range(16):
            w_v[rows_of(k, n), 0:128] = (-NODE_W[n] * (d1[n] + d2[n])).astype(jnp.bfloat16)
    sent = jnp.dot(s_v[...], w_v[:, 0:256], preferred_element_type=jnp.float32)
    out_b[0] = sent[:, 0:128]
    spread(4)

    def send(fields, groups):
        for f in fields:
            for g in groups:
                remote(f, g).start()

    def second_pass(k, carry):
        u1, u2, phi = fields_of(k)
        energy, cov1, cov2 = [], [], []
        for n in range(16):
            rows = rows_of(k, n)
            energy.append(0.5 * (u1[n] * u1[n] + u2[n] * u2[n]) + phi[n])
            cov1.append(co_v[3, rows, :] * u1[n] - co_v[2, rows, :] * u2[n])
            cov2.append(co_v[0, rows, :] * u2[n] - co_v[1, rows, :] * u1[n])
        curl1 = along_cols(cov2)
        curl2 = along_rows(cov1)
        e1 = along_cols(energy)
        e2 = along_rows(energy)
        for n in range(16):
            rows = rows_of(k, n)
            eta = NODE_W[n] * (curl1[n] - curl2[n]) + co_v[4, rows, :]
            grad1 = co_v[0, rows, :] * e1[n] + co_v[2, rows, :] * e2[n]
            grad2 = co_v[1, rows, :] * e1[n] + co_v[3, rows, :] * e2[n]
            w_v[rows, 256:384] = (eta * u2[n] - NODE_W[n] * grad1).astype(jnp.bfloat16)
            w_v[rows, 384:512] = (-eta * u1[n] - NODE_W[n] * grad2).astype(jnp.bfloat16)
        return carry

    def wind():
        lax.fori_loop(0, BLOCKS, second_pass, 0)
        sent = jnp.dot(s_v[...], w_v[:, 256:512], preferred_element_type=jnp.float32)
        for f in (1, 2):
            out_b[f] = sent[:, 128 * (f - 1) : 128 * f]

    def table(i, carry):
        x = pltpu.roll(ids_v[...], LEV - 8 * i, 1)
        for lane in range(8):
            col = jnp.broadcast_to(x[:, lane : lane + 1], (16, LEV))
            rows = pl.ds(pl.multiple_of(i * 128 + lane * 16, 16), 16)
            for j in range(8):
                a_v[rows, 128 * j : 128 * j + 128] = one_hot(col, id_rows[j])
            for chunk in range(2):
                r_v[rows, 128 * chunk : 128 * chunk + 128] = one_hot(
                    col, recv_row[0:1, 128 * chunk : 128 * chunk + 128]
                )
        return carry

    def tables():
        lax.fori_loop(0, ELEMS // 8, table, 0)

    def gather(i, carry):
        rows = pl.ds(pl.multiple_of(i * 256, 256), 256)
        acc_v[rows, :] = jnp.dot(a_v[rows, :], w_v[...], preferred_element_type=jnp.float32)
        return carry

    def sums():
        lax.fori_loop(0, NODES // 256, gather, 0)

    face = lax.axis_index("face")
    plane = lax.rem(face // 2, PLANES)
    first = plane < 4

    @pl.when(first)
    def _():
        wind()
        tables()
        sums()

    pl.semaphore_wait(barrier, len(offsets))
    send((0,), GROUPS)
    weight = sent[:, 128:256]
    weight = weight + pltpu.roll(weight, 64, 1)
    diagonal = lax.broadcasted_iota(jnp.int32, (128, 128), 0) == lane_iota((128, 128))
    for chunk in range(2):
        out_w[chunk] = jnp.sum(
            jnp.where(diagonal, weight[128 * chunk : 128 * chunk + 128], 0.0), axis=0, keepdims=True
        )
    for g in GROUPS:
        remote_weights(g).start()

    @pl.when(first)
    def _():
        send((1, 2), GROUPS)

    @pl.when(jnp.logical_not(first))
    def _():
        turn = lax.rem(plane, 2) * 2 + 1 - lax.rem(face, 2)
        wind()
        pl.when(turn == 0)(lambda: send((1, 2), GROUPS[:2]))
        send((1, 2), GROUPS[2:])
        tables()
        pl.when((turn == 1) | (turn == 2))(lambda: send((1, 2), GROUPS[:2]))
        sums()
        pl.when(turn == 3)(lambda: send((1, 2), GROUPS[:2]))

    columns = (slice(0, 128), slice(256, 384), slice(384, 512))

    def finish(f):
        got = jnp.dot(
            r_v[...], in_b[f].astype(jnp.bfloat16), preferred_element_type=jnp.float32
        )
        out_ref[(f + 2) % 3] = (acc_v[:, columns[f]] + got * inv_v[...]).astype(jnp.bfloat16)

    for g in GROUPS:
        remote_weights(g).wait_recv()
    lane = lane_iota((1, 128))
    low = lane_iota((128, 128)) < 64
    blocks = []
    for chunk in range(2):
        row = jnp.zeros((1, 128), jnp.float32)
        for group, _, count, first in GROUPS:
            if first // 128 == chunk:
                at = first % 128
                row = jnp.where((lane >= at) & (lane < at + count), in_w[group], row)
        col = jnp.transpose(jnp.broadcast_to(row, (128, 128)))
        high = col.astype(jnp.bfloat16).astype(jnp.float32)
        blocks.append(jnp.where(low, high, col - high).astype(jnp.bfloat16))
    arrived = jnp.concatenate(blocks, axis=0)

    weight = jnp.dot(r_v[...], arrived, preferred_element_type=jnp.float32) + acc_v[:, 128:256]
    inv_v[...] = STEP_SIZE / (weight + pltpu.roll(weight, 64, 1))
    for f in range(3):
        field = prog_v[(f + 2) % 3].astype(jnp.float32)
        acc_v[:, columns[f]] = field + acc_v[:, columns[f]] * inv_v[...]
    for f in range(3):
        for g in GROUPS:
            remote(f, g).wait_recv()
        finish(f)
    for g in GROUPS:
        for f in range(3):
            remote(f, g).wait_send()
        remote_weights(g).wait_send()


def solution(mesh):
    sizes = (mesh.shape["face"], mesh.shape["sub"])

    def local(prognostic, metric, coriolis, node_point, send_point, recv_point):
        result = pl.pallas_call(
            functools.partial(kernel, sizes),
            out_shape=pltpu.VMEM((3, NODES, LEV), jnp.bfloat16),
            in_specs=[pl.BlockSpec(memory_space=pltpu.HBM)] * 6,
            out_specs=pl.BlockSpec(memory_space=pltpu.VMEM),
            scratch_shapes=[
                pltpu.VMEM((3, NODES, LEV), jnp.bfloat16),
                pltpu.VMEM((4, 16, ELEMS), jnp.float32),
                pltpu.VMEM((16, ELEMS), jnp.float32),
                pltpu.VMEM((16, ELEMS), jnp.int32),
                pltpu.VMEM((1, LINKS), jnp.int32),
                pltpu.VMEM((1, LINKS), jnp.int32),
                pltpu.VMEM((NODES, 3 * LEV), jnp.float32),
                pltpu.VMEM((BROWS, BROWS), jnp.bfloat16),
                pltpu.VMEM((ELEMS, 128), jnp.float32),
                pltpu.VMEM((5, NODES, LEV), jnp.float32),
                pltpu.VMEM((NODES, 512), jnp.bfloat16),
                pltpu.VMEM((ROWS, NODES), jnp.bfloat16),
                pltpu.VMEM((NODES, NODES), jnp.bfloat16),
                pltpu.VMEM((NODES, ROWS), jnp.bfloat16),
                pltpu.VMEM((NODES, 512), jnp.float32),
                pltpu.VMEM((NODES, LEV), jnp.float32),
                pltpu.VMEM((16, LEV), jnp.int32),
                pltpu.VMEM((3, ROWS, LEV), jnp.float32),
                pltpu.VMEM((3, ROWS, LEV), jnp.float32),
                pltpu.VMEM((2, 1, LEV), jnp.float32),
                pltpu.VMEM((8, 1, LEV), jnp.float32),
                pltpu.SemaphoreType.DMA((11,)),
                pltpu.SemaphoreType.DMA((4, 8)),
                pltpu.SemaphoreType.DMA((4, 8)),
            ],
            compiler_params=pltpu.CompilerParams(
                collective_id=0, has_side_effects=True, vmem_limit_bytes=40 * 1024 * 1024
            ),
        )(
            pltpu.with_memory_space_constraint(prognostic.reshape(3, NODES, LEV), pltpu.HBM),
            pltpu.with_memory_space_constraint(jnp.transpose(metric, (0, 2, 1)), pltpu.HBM),
            pltpu.with_memory_space_constraint(jnp.transpose(coriolis), pltpu.HBM),
            pltpu.with_memory_space_constraint(jnp.transpose(node_point), pltpu.HBM),
            pltpu.with_memory_space_constraint(send_point.reshape(1, LINKS), pltpu.HBM),
            pltpu.with_memory_space_constraint(recv_point.reshape(1, LINKS), pltpu.HBM),
        )
        return result.reshape(3, ELEMS, 16, LEV)

    placed = (
        P(None, ("face", "sub"), None, None),
        P(None, ("face", "sub"), None),
        P(("face", "sub"), None),
        P(("face", "sub"), None),
        P(("face", "sub")),
        P(("face", "sub")),
    )
    return jax.shard_map(
        local,
        mesh=mesh,
        in_specs=placed,
        out_specs=P(None, ("face", "sub"), None, None),
        check_vma=False,
    )
```

```python
import functools
import math

import jax
import jax.numpy as jnp
import numpy as np
from jax import lax
from jax.experimental import pallas as pl
from jax.experimental.pallas import tpu as pltpu
from jax.sharding import PartitionSpec as P

MESH = pl.DeviceIdType.MESH
BX = 32
BY = 2
ELEMS = BX * BY
NODES = ELEMS * 16
LEV = 128
SIDE = 3 * BY + 1
TOP = 3 * BX + 1
LINKS = 2 * SIDE + 2 * TOP + 4
STEP_SIZE = 0.1
BLK = 16
BLOCKS = ELEMS // BLK
HALF = NODES // 2
MASS = 5
PLANES = 16
BROWS = 16 * BLK

GROUPS = (
    (2, 2 * SIDE, TOP, 0),
    (3, 2 * SIDE + TOP, TOP, 128),
    (0, 0, SIDE, 104),
    (1, SIDE, SIDE, 232),
    (4, 2 * SIDE + 2 * TOP, 1, 112),
    (5, 2 * SIDE + 2 * TOP + 1, 1, 240),
    (6, 2 * SIDE + 2 * TOP + 2, 1, 120),
    (7, 2 * SIDE + 2 * TOP + 3, 1, 248),
)
ROWS = 256


def gll_tables():
    abscissa = np.array([-1.0, -math.sqrt(0.2), math.sqrt(0.2), 1.0])
    legendre = 0.5 * (5.0 * abscissa * abscissa * abscissa - 3.0 * abscissa)
    derivative = np.zeros((4, 4))
    for target in range(4):
        for source in range(4):
            if target != source:
                derivative[target, source] = legendre[target] / (
                    legendre[source] * (abscissa[target] - abscissa[source])
                )
    derivative[0, 0] = -3.0
    derivative[3, 3] = 3.0
    weights = np.array([1.0, 5.0, 5.0, 1.0]) / 6.0
    return derivative, weights


DERIV, GLL = gll_tables()
EV0 = float(0.5 * (DERIV[0, 0] + DERIV[0, 3]))
EV1 = float(0.5 * (DERIV[1, 0] + DERIV[1, 3]))
OD00 = float(0.5 * (DERIV[0, 0] - DERIV[0, 3]))
OD01 = float(0.5 * (DERIV[0, 1] - DERIV[0, 2]))
OD10 = float(0.5 * (DERIV[1, 0] - DERIV[1, 3]))
OD11 = float(0.5 * (DERIV[1, 1] - DERIV[1, 2]))


def derive4(s):
    o0 = s[0] - s[3]
    o1 = s[1] - s[2]
    q = (s[0] + s[3]) - (s[1] + s[2])
    h0 = OD00 * o0 + OD01 * o1
    h1 = OD10 * o0 + OD11 * o1
    g0 = EV0 * q
    g1 = EV1 * q
    return [h0 + g0, h1 + g1, h1 - g1, h0 - g0]


def along_cols(s):
    out = []
    for r in range(4):
        out += derive4(s[4 * r : 4 * r + 4])
    return out


def along_rows(s):
    out = [None] * 16
    for c in range(4):
        for r, value in enumerate(derive4(s[c::4])):
            out[4 * r + c] = value
    return out


NODE_W = [float(GLL[n // 4] * GLL[n % 4]) for n in range(16)]


def lane_iota(shape):
    return lax.broadcasted_iota(jnp.int32, shape, len(shape) - 1)


def padded_slots(ref):
    x = jnp.concatenate(
        [jnp.broadcast_to(ref[...], (8, LINKS)), jnp.full((8, ROWS - LINKS), -1, jnp.int32)], axis=1
    )
    lane = lane_iota((8, ROWS))
    out = jnp.full((8, ROWS), -1, jnp.int32)
    for _, first, count, row in GROUPS:
        moved = pltpu.roll(x, (row - first) % ROWS, 1)
        out = jnp.where((lane >= row) & (lane < row + count), moved, out)
    return out


def one_hot(col, row):
    return jnp.where(col == row, 1.0, 0.0).astype(jnp.bfloat16)


def kernel(
    sizes,
    prog_hbm, met_hbm, cor_hbm, np_hbm, sp_hbm, rp_hbm,
    out_ref,
    prog_v, met_v, cor_v, np_v, sp_v, rp_v,
    f_v, turn_v, ct_v, co_v, w_v, s_v, a_v, r_v, acc_v, inv_v, ids_v, out_b, in_b, out_w, in_w,
    in_sem, send_sem, recv_sem,
):
    n_face, n_sub = sizes
    total = n_face * n_sub
    lap = 4 * n_sub
    offsets = (1, -1, lap, -lap, lap + 1, -lap - 1, lap - 1, 1 - lap)
    me = lax.axis_index("face") * n_sub + lax.axis_index("sub")

    def device(offset):
        t = lax.rem(me + (offset + total), total)
        return (t // n_sub, lax.rem(t, n_sub))

    barrier = pltpu.get_barrier_semaphore()
    for group in (2, 4, 6, 3, 5, 7, 0, 1):
        offset = offsets[group]
        pl.semaphore_signal(barrier, inc=1, device_id=device(offset), device_id_type=MESH)
    loads = []
    for i, (src, dst) in enumerate(
        ((np_hbm, np_v), (sp_hbm, sp_v), (rp_hbm, rp_v), (met_hbm, met_v), (cor_hbm, cor_v))
    ):
        loads.append(pltpu.make_async_copy(src, dst, in_sem.at[i]))
    for h in range(2):
        rows = pl.ds(HALF * h, HALF)
        for f in range(3):
            loads.append(
                pltpu.make_async_copy(
                    prog_hbm.at[f, rows], prog_v.at[f, rows], in_sem.at[5 + 3 * h + f]
                )
            )
    for load in loads:
        load.start()

    def remote(f, g):
        group, _, count, row = g
        return pltpu.make_async_remote_copy(
            src_ref=out_b.at[f, pl.ds(row, count)],
            dst_ref=in_b.at[f, pl.ds(row, count)],
            send_sem=send_sem.at[f, group],
            recv_sem=recv_sem.at[f, group],
            device_id=device(offsets[group]),
            device_id_type=MESH,
        )

    def remote_weights(g):
        group, _, _, row = g
        return pltpu.make_async_remote_copy(
            src_ref=out_w.at[row // 128],
            dst_ref=in_w.at[group],
            send_sem=send_sem.at[3, group],
            recv_sem=recv_sem.at[3, group],
            device_id=device(offsets[group]),
            device_id_type=MESH,
        )

    edges = sorted((row, row + count) for _, _, count, row in GROUPS)
    for f in range(3):
        for (_, end), nxt in zip(edges, [e[0] for e in edges[1:]] + [ROWS]):
            in_b[f, end:nxt, :] = jnp.zeros((nxt - end, LEV), jnp.float32)

    for load in loads[:3]:
        load.wait()
    ids = np_v[...]
    ids2 = jnp.concatenate([ids, ids], axis=1)
    ids_v[...] = ids2
    rolled = [ids2 if i == 0 else pltpu.roll(ids2, 16 * i, 1) for i in range(4)]
    sub = lax.broadcasted_iota(jnp.int32, (8, LEV), 0)
    own = sub == lane_iota((8, LEV)) // BLK
    id_rows = []
    for k in range(BLOCKS):
        for h in range(2):
            pick = rolled[(-k) % 4][8 * h : 8 * h + 8]
            for i in range(1, 4):
                pick = jnp.where(sub % 4 == i, rolled[(i - k) % 4][8 * h : 8 * h + 8], pick)
            id_rows.append(jnp.sum(jnp.where(own, pick, 0), axis=0, keepdims=True))
    send_row = padded_slots(sp_v)
    recv_row = padded_slots(rp_v)
    for chunk in range(2):
        col = jnp.transpose(
            jnp.broadcast_to(send_row[0:1, 128 * chunk : 128 * chunk + 128], (128, 128))
        )
        for j in range(8):
            s_v[128 * chunk : 128 * chunk + 128, 128 * j : 128 * j + 128] = one_hot(col, id_rows[j])

    for load in loads[3:5]:
        load.wait()
    m_a, m_b, m_e, m_g = (met_v[i] for i in range(4))
    inverse = 1.0 / (m_a * m_g - m_b * m_e)
    node = lax.broadcasted_iota(jnp.int32, (16, ELEMS), 0)
    wr = jnp.where((node < 4) | (node >= 12), float(GLL[0]), float(GLL[1]))
    wc = jnp.where((node % 4 == 0) | (node % 4 == 3), float(GLL[0]), float(GLL[1]))
    mass = wr * wc * inverse
    coefs = jnp.concatenate(
        [m_a * inverse, m_b * inverse, m_e * inverse, m_g * inverse, mass * cor_v[...], mass, mass, mass],
        axis=0,
    )
    ct_v[...] = jnp.transpose(coefs)

    def rows_of(k, n):
        first = k * BROWS + n * BLK
        return pl.ds(first if isinstance(first, int) else pl.multiple_of(first, BLK), BLK)

    at = lax.broadcasted_iota(jnp.int32, (BROWS, BROWS), 0)
    turn_v[...] = one_hot(at % BLK * 16 + at // BLK, lane_iota((BROWS, BROWS)))

    def spread(q):
        for n in range(16):
            wide = jnp.broadcast_to(ct_v[:, q * 16 + n : q * 16 + n + 1], (ELEMS, LEV))
            if q == MASS:
                high = wide.astype(jnp.bfloat16).astype(jnp.float32)
                low = lane_iota((ELEMS, LEV)) >= 64
                wide = jnp.where(low, wide - high, high).astype(jnp.bfloat16)
            for k in range(BLOCKS):
                part = wide[BLK * k : BLK * k + BLK]
                if q == MASS:
                    w_v[rows_of(k, n), 128:256] = part
                else:
                    co_v[q, rows_of(k, n), :] = part

    def turn_half(h):
        for load in loads[5 + 3 * h : 8 + 3 * h]:
            load.wait()
        for k in (2 * h, 2 * h + 1):
            rows = slice(BROWS * k, BROWS * k + BROWS)
            block = jnp.concatenate([prog_v[f, rows] for f in range(3)], axis=1)
            f_v[rows, :] = jnp.dot(turn_v[...], block, preferred_element_type=jnp.float32)

    spread(0)
    spread(1)
    turn_half(0)
    spread(2)
    spread(3)
    spread(MASS)
    turn_half(1)

    def fields_of(k):
        return [
            [f_v[rows_of(k, n), LEV * f : LEV * f + LEV] for n in range(16)] for f in range(3)
        ]

    for k in range(BLOCKS):
        u1, u2, phi = fields_of(k)
        con1, con2 = [], []
        for n in range(16):
            f1 = phi[n] * u1[n]
            f2 = phi[n] * u2[n]
            con1.append(co_v[0, rows_of(k, n), :] * f1 + co_v[1, rows_of(k, n), :] * f2)
            con2.append(co_v[2, rows_of(k, n), :] * f1 + co_v[3, rows_of(k, n), :] * f2)
        d1 = along_cols(con1)
        d2 = along_rows(con2)
        for n in range(16):
            w_v[rows_of(k, n), 0:128] = (-NODE_W[n] * (d1[n] + d2[n])).astype(jnp.bfloat16)
    sent = jnp.dot(s_v[...], w_v[:, 0:256], preferred_element_type=jnp.float32)
    out_b[0] = sent[:, 0:128]
    spread(4)

    def send(fields, groups):
        for f in fields:
            for g in groups:
                remote(f, g).start()

    def second_pass(k, carry):
        u1, u2, phi = fields_of(k)
        energy, cov1, cov2 = [], [], []
        for n in range(16):
            rows = rows_of(k, n)
            energy.append(0.5 * (u1[n] * u1[n] + u2[n] * u2[n]) + phi[n])
            cov1.append(co_v[3, rows, :] * u1[n] - co_v[2, rows, :] * u2[n])
            cov2.append(co_v[0, rows, :] * u2[n] - co_v[1, rows, :] * u1[n])
        curl1 = along_cols(cov2)
        curl2 = along_rows(cov1)
        e1 = along_cols(energy)
        e2 = along_rows(energy)
        for n in range(16):
            rows = rows_of(k, n)
            eta = NODE_W[n] * (curl1[n] - curl2[n]) + co_v[4, rows, :]
            grad1 = co_v[0, rows, :] * e1[n] + co_v[2, rows, :] * e2[n]
            grad2 = co_v[1, rows, :] * e1[n] + co_v[3, rows, :] * e2[n]
            w_v[rows, 256:384] = (eta * u2[n] - NODE_W[n] * grad1).astype(jnp.bfloat16)
            w_v[rows, 384:512] = (-eta * u1[n] - NODE_W[n] * grad2).astype(jnp.bfloat16)
        return carry

    def wind():
        lax.fori_loop(0, BLOCKS, second_pass, 0)
        sent = jnp.dot(s_v[...], w_v[:, 256:512], preferred_element_type=jnp.float32)
        for f in (1, 2):
            out_b[f] = sent[:, 128 * (f - 1) : 128 * f]

    def table(i, carry):
        x = pltpu.roll(ids_v[...], LEV - 8 * i, 1)
        for lane in range(8):
            col = jnp.broadcast_to(x[:, lane : lane + 1], (16, LEV))
            rows = pl.ds(pl.multiple_of(i * 128 + lane * 16, 16), 16)
            for j in range(8):
                a_v[rows, 128 * j : 128 * j + 128] = one_hot(col, id_rows[j])
            for chunk in range(2):
                r_v[rows, 128 * chunk : 128 * chunk + 128] = one_hot(
                    col, recv_row[0:1, 128 * chunk : 128 * chunk + 128]
                )
        return carry

    def tables():
        lax.fori_loop(0, ELEMS // 8, table, 0)

    def gather(i, carry):
        rows = pl.ds(pl.multiple_of(i * 256, 256), 256)
        acc_v[rows, :] = jnp.dot(a_v[rows, :], w_v[...], preferred_element_type=jnp.float32)
        return carry

    def sums():
        lax.fori_loop(0, NODES // 256, gather, 0)

    face = lax.axis_index("face")
    plane = lax.rem(face // 2, PLANES)
    first = plane < 4

    @pl.when(first)
    def _():
        wind()
        tables()
        sums()

    pl.semaphore_wait(barrier, len(offsets))
    send((0,), GROUPS[:2])
    weight = sent[:, 128:256]
    weight = weight + pltpu.roll(weight, 64, 1)
    diagonal = lax.broadcasted_iota(jnp.int32, (128, 128), 0) == lane_iota((128, 128))
    for chunk in range(2):
        out_w[chunk] = jnp.sum(
            jnp.where(diagonal, weight[128 * chunk : 128 * chunk + 128], 0.0), axis=0, keepdims=True
        )
    def send_weights(groups):
        for g in groups:
            remote_weights(g).start()

    send_weights(GROUPS[:2])

    @pl.when(first)
    def _():
        send((0,), GROUPS[2:])
        send_weights(GROUPS[2:])
        send((1, 2), GROUPS)

    @pl.when(jnp.logical_not(first))
    def _():
        turn = lax.rem(plane, 2) * 2 + 1 - lax.rem(face, 2)
        wind()
        pl.when(turn == 0)(lambda: send((1, 2), GROUPS[:2]))
        send_weights(GROUPS[2:])
        send((0, 1, 2), GROUPS[2:])
        tables()
        pl.when((turn == 1) | (turn == 2))(lambda: send((1, 2), GROUPS[:2]))
        sums()
        pl.when(turn == 3)(lambda: send((1, 2), GROUPS[:2]))

    columns = (slice(0, 128), slice(256, 384), slice(384, 512))

    def finish(f):
        got = jnp.dot(
            r_v[...], in_b[f].astype(jnp.bfloat16), preferred_element_type=jnp.float32
        )
        out_ref[(f + 2) % 3] = (acc_v[:, columns[f]] + got * inv_v[...]).astype(jnp.bfloat16)

    for g in GROUPS:
        remote_weights(g).wait_recv()
    lane = lane_iota((1, 128))
    low = lane_iota((128, 128)) < 64
    blocks = []
    for chunk in range(2):
        row = jnp.zeros((1, 128), jnp.float32)
        for group, _, count, first in GROUPS:
            if first // 128 == chunk:
                at = first % 128
                row = jnp.where((lane >= at) & (lane < at + count), in_w[group], row)
        col = jnp.transpose(jnp.broadcast_to(row, (128, 128)))
        high = col.astype(jnp.bfloat16).astype(jnp.float32)
        blocks.append(jnp.where(low, high, col - high).astype(jnp.bfloat16))
    arrived = jnp.concatenate(blocks, axis=0)

    weight = jnp.dot(r_v[...], arrived, preferred_element_type=jnp.float32) + acc_v[:, 128:256]
    inv_v[...] = STEP_SIZE / (weight + pltpu.roll(weight, 64, 1))
    for f in range(3):
        field = prog_v[(f + 2) % 3].astype(jnp.float32)
        acc_v[:, columns[f]] = field + acc_v[:, columns[f]] * inv_v[...]
    for f in range(3):
        for g in GROUPS:
            remote(f, g).wait_recv()
        finish(f)
    for g in GROUPS:
        for f in range(3):
            remote(f, g).wait_send()
        remote_weights(g).wait_send()


def solution(mesh):
    sizes = (mesh.shape["face"], mesh.shape["sub"])

    def local(prognostic, metric, coriolis, node_point, send_point, recv_point):
        result = pl.pallas_call(
            functools.partial(kernel, sizes),
            out_shape=pltpu.VMEM((3, NODES, LEV), jnp.bfloat16),
            in_specs=[pl.BlockSpec(memory_space=pltpu.HBM)] * 6,
            out_specs=pl.BlockSpec(memory_space=pltpu.VMEM),
            scratch_shapes=[
                pltpu.VMEM((3, NODES, LEV), jnp.bfloat16),
                pltpu.VMEM((4, 16, ELEMS), jnp.float32),
                pltpu.VMEM((16, ELEMS), jnp.float32),
                pltpu.VMEM((16, ELEMS), jnp.int32),
                pltpu.VMEM((1, LINKS), jnp.int32),
                pltpu.VMEM((1, LINKS), jnp.int32),
                pltpu.VMEM((NODES, 3 * LEV), jnp.float32),
                pltpu.VMEM((BROWS, BROWS), jnp.bfloat16),
                pltpu.VMEM((ELEMS, 128), jnp.float32),
                pltpu.VMEM((5, NODES, LEV), jnp.float32),
                pltpu.VMEM((NODES, 512), jnp.bfloat16),
                pltpu.VMEM((ROWS, NODES), jnp.bfloat16),
                pltpu.VMEM((NODES, NODES), jnp.bfloat16),
                pltpu.VMEM((NODES, ROWS), jnp.bfloat16),
                pltpu.VMEM((NODES, 512), jnp.float32),
                pltpu.VMEM((NODES, LEV), jnp.float32),
                pltpu.VMEM((16, LEV), jnp.int32),
                pltpu.VMEM((3, ROWS, LEV), jnp.float32),
                pltpu.VMEM((3, ROWS, LEV), jnp.float32),
                pltpu.VMEM((2, 1, LEV), jnp.float32),
                pltpu.VMEM((8, 1, LEV), jnp.float32),
                pltpu.SemaphoreType.DMA((11,)),
                pltpu.SemaphoreType.DMA((4, 8)),
                pltpu.SemaphoreType.DMA((4, 8)),
            ],
            compiler_params=pltpu.CompilerParams(
                collective_id=0, has_side_effects=True, vmem_limit_bytes=40 * 1024 * 1024
            ),
        )(
            pltpu.with_memory_space_constraint(prognostic.reshape(3, NODES, LEV), pltpu.HBM),
            pltpu.with_memory_space_constraint(jnp.transpose(metric, (0, 2, 1)), pltpu.HBM),
            pltpu.with_memory_space_constraint(jnp.transpose(coriolis), pltpu.HBM),
            pltpu.with_memory_space_constraint(jnp.transpose(node_point), pltpu.HBM),
            pltpu.with_memory_space_constraint(send_point.reshape(1, LINKS), pltpu.HBM),
            pltpu.with_memory_space_constraint(recv_point.reshape(1, LINKS), pltpu.HBM),
        )
        return result.reshape(3, ELEMS, 16, LEV)

    placed = (
        P(None, ("face", "sub"), None, None),
        P(None, ("face", "sub"), None),
        P(("face", "sub"), None),
        P(("face", "sub"), None),
        P(("face", "sub")),
        P(("face", "sub")),
    )
    return jax.shard_map(
        local,
        mesh=mesh,
        in_specs=placed,
        out_specs=P(None, ("face", "sub"), None, None),
        check_vma=False,
    )
```
